32 devices in a mesh: rep: 1 (over z), dp: 32 (over x, y, core).
Axes of the slice: x: 4, y: 4, z: 1, core: 2. Of those that a mesh axis runs over, the one named last changes fastest.
The devices are a block of a 4x4x8 slice.
Arguments:
- x: bfloat16 [32, 1024, 512], P(('rep', 'dp'))
- dy: bfloat16 [32, 1024, 512], P(('rep', 'dp'))
- wq: bfloat16 [2, 512, 2048], P(None, 'dp')
- wk: bfloat16 [2, 512, 2048], P(None, 'dp')
- wv: bfloat16 [2, 512, 2048], P(None, 'dp')
- wo: bfloat16 [2, 2048, 512], P(None, 'dp')
- w_gate: bfloat16 [2, 512, 8192], P(None, 'dp')
- w_up: bfloat16 [2, 512, 8192], P(None, 'dp')
- w_down: bfloat16 [2, 8192, 512], P(None, 'dp')
- m_wq: float32 [2, 512, 2048], P(None, 'dp')
- m_wk: float32 [2, 512, 2048], P(None, 'dp')
- m_wv: float32 [2, 512, 2048], P(None, 'dp')
- m_wo: float32 [2, 2048, 512], P(None, 'dp')
- m_w_gate: float32 [2, 512, 8192], P(None, 'dp')
- m_w_up: float32 [2, 512, 8192], P(None, 'dp')
- m_w_down: float32 [2, 8192, 512], P(None, 'dp')
- v_wq: float32 [2, 512, 2048], P(None, 'dp')
- v_wk: float32 [2, 512, 2048], P(None, 'dp')
- v_wv: float32 [2, 512, 2048], P(None, 'dp')
- v_wo: float32 [2, 2048, 512], P(None, 'dp')
- v_w_gate: float32 [2, 512, 8192], P(None, 'dp')
- v_w_up: float32 [2, 512, 8192], P(None, 'dp')
- v_w_down: float32 [2, 8192, 512], P(None, 'dp')
Outputs:
- output 1: bfloat16 [2, 512, 2048], P('rep', 'dp')
- output 2: bfloat16 [2, 512, 2048], P('rep', 'dp')
- output 3: bfloat16 [2, 512, 2048], P('rep', 'dp')
- output 4: bfloat16 [2, 2048, 512], P('rep', 'dp')
- output 5: bfloat16 [2, 512, 8192], P('rep', 'dp')
- output 6: bfloat16 [2, 512, 8192], P('rep', 'dp')
- output 7: bfloat16 [2, 8192, 512], P('rep', 'dp')
- output 8: float32 [2, 512, 2048], P('rep', 'dp')
- output 9: float32 [2, 512, 2048], P('rep', 'dp')
- output 10: float32 [2, 512, 2048], P('rep', 'dp')
- output 11: float32 [2, 2048, 512], P('rep', 'dp')
- output 12: float32 [2, 512, 8192], P('rep', 'dp')
- output 13: float32 [2, 512, 8192], P('rep', 'dp')
- output 14: float32 [2, 8192, 512], P('rep', 'dp')
- output 15: float32 [2, 512, 2048], P('rep', 'dp')
- output 16: float32 [2, 512, 2048], P('rep', 'dp')
- output 17: float32 [2, 512, 2048], P('rep', 'dp')
- output 18: float32 [2, 2048, 512], P('rep', 'dp')
- output 19: float32 [2, 512, 8192], P('rep', 'dp')
- output 20: float32 [2, 512, 8192], P('rep', 'dp')
- output 21: float32 [2, 8192, 512], P('rep', 'dp')
All inputs are finite; a program needn't handle non-finite values.
Results may differ from the reference program's by a relative error of at most 0.024.
Values are sent between devices in bfloat16 or wider.
A program may use at most 768 MiB of HBM per device.

```python
import jax
import jax.numpy as jnp
from jax import lax

SEQUENCES = 32
TOKENS = 1024
D = 512
HEADS = 16
KV_HEADS = 16
HEAD = 128
FF = 8192
LAYERS = 2
THETA = 10000
NAMES = ("wq", "wk", "wv", "wo", "w_gate", "w_up", "w_down")
SHAPES = {
    "wq": (LAYERS, D, HEADS * HEAD),
    "wk": (LAYERS, D, KV_HEADS * HEAD),
    "wv": (LAYERS, D, KV_HEADS * HEAD),
    "wo": (LAYERS, HEADS * HEAD, D),
    "w_gate": (LAYERS, D, FF),
    "w_up": (LAYERS, D, FF),
    "w_down": (LAYERS, FF, D),
}


def bump(key, n, height):
    away = (jnp.arange(n, dtype=jnp.int32) - jax.random.randint(key, (), 0, n, jnp.int32)) % n
    return jnp.where(away < n // 8, height, 1.0)


def together(key, own, strength):
    shared = jax.random.normal(key, own.shape[1:], jnp.float32)
    return (own + strength * shared) * lax.rsqrt(1 + strength * strength)


def setup_inputs(seed: int = 0, part: int = 0) -> dict:
    kx, kdy, ka, kb, kz, kf, kh, kl, *keys = jax.random.split(jax.random.key(seed), 8 + 3 * len(NAMES))
    kx, kdy, ka, kb = (jax.random.fold_in(k, part) for k in (kx, kdy, ka, kb))
    kw, km, kv = (keys[i::3] for i in range(3))
    shape = (SEQUENCES, TOKENS, D)
    much_x, much_dy = jax.random.uniform(kz, (2,), jnp.float32, 0.0, 1.0)
    loud = 2.0 ** jax.random.uniform(jax.random.fold_in(kz, 1), (), jnp.float32, -1.0, 2.0)
    layers = 2.0 ** jax.random.uniform(kl, (LAYERS, 1, 1), jnp.float32, -1.0, 1.0)
    times = {"wq": 1.0, "wk": 1.0, "wv": 2.0, "wo": layers, "w_gate": 1.0, "w_up": bump(kh, FF, 4.0), "w_down": layers}
    x = together(ka, jax.random.normal(kx, shape, jnp.float32), much_x) * bump(kf, D, 4.0)
    dy = together(kb, jax.random.normal(kdy, shape, jnp.float32), much_dy)
    drawn = {"x": x.astype(jnp.bfloat16), "dy": (loud * dy * (SEQUENCES * TOKENS) ** -0.5).astype(jnp.bfloat16)}
    for key, name in zip(kw, NAMES, strict=True):
        drawn[name] = (jax.random.normal(key, SHAPES[name], jnp.float32) * SHAPES[name][1] ** -0.5 * times[name]).astype(jnp.bfloat16)
    for key, name in zip(km, NAMES, strict=True):
        drawn[f"m_{name}"] = 0.1 * jax.random.normal(key, SHAPES[name], jnp.float32)
    for key, name in zip(kv, NAMES, strict=True):
        drawn[f"v_{name}"] = jax.random.uniform(key, SHAPES[name], jnp.float32, 0.02, 0.06)
    return drawn


def matmul(a, w):
    return jnp.dot(a, w, preferred_element_type=jnp.float32).astype(jnp.bfloat16)


def normed(h):
    wide = h.astype(jnp.float32)
    scale = lax.rsqrt(jnp.mean(wide**2, -1, keepdims=True) + 1e-6)
    return (wide * scale).astype(jnp.bfloat16)


def turned(t, theta):
    half = t.shape[-1] // 2
    angle = jnp.arange(t.shape[0], dtype=jnp.float32)[:, None] * theta ** (-jnp.arange(half, dtype=jnp.float32) / half)
    cos, sin = jnp.cos(angle)[:, None], jnp.sin(angle)[:, None]
    a, b = t[..., :half].astype(jnp.float32), t[..., half:].astype(jnp.float32)
    return jnp.concatenate([a * cos - b * sin, b * cos + a * sin], -1).astype(jnp.bfloat16)


def seen_by(q, k, v):
    tokens, kv = q.shape[0], k.shape[1]
    q = q.reshape(tokens, kv, -1, q.shape[-1])
    scores = jnp.einsum("tgsd,ugd->gstu", q.astype(jnp.float32), k.astype(jnp.float32)) * q.shape[-1] ** -0.5
    place = jnp.arange(tokens)
    weights = jax.nn.softmax(jnp.where(place[:, None] >= place, scores, -jnp.inf), -1).astype(jnp.bfloat16)
    return jnp.einsum("gstu,ugd->tgsd", weights.astype(jnp.float32), v.astype(jnp.float32)).astype(jnp.bfloat16).reshape(tokens, -1)


def layer(h, w):
    a = normed(h)
    q, k = (turned(matmul(a, w[name]).reshape(h.shape[0], -1, HEAD), THETA) for name in ("wq", "wk"))
    h = h + matmul(seen_by(q, k, matmul(a, w["wv"]).reshape(h.shape[0], -1, HEAD)), w["wo"])
    b = normed(h)
    gate = jnp.dot(b, w["w_gate"], preferred_element_type=jnp.float32)
    up = jnp.dot(b, w["w_up"], preferred_element_type=jnp.float32)
    return h + matmul((jax.nn.silu(gate) * up).astype(jnp.bfloat16), w["w_down"])


def adamw(w, m, v, g):
    m = 0.9 * m + 0.1 * g
    v = 0.95 * v + 0.05 * g * g
    step = m * lax.rsqrt(v + 1e-8) + 0.1 * w
    return (w - 0.02 * step).astype(jnp.bfloat16), m, v


def clipped(gradients, sum_of_squares, count):
    factor = jnp.minimum(1.0, 0.5 * lax.rsqrt(sum_of_squares / count + 1e-30))
    return [g * factor for g in gradients]


def stack(weights, h):
    return lax.scan(lambda h, w: (layer(h, w), None), h, weights)[0]


def reference(x, dy, wq, wk, wv, wo, w_gate, w_up, w_down, m_wq, m_wk, m_wv, m_wo, m_w_gate, m_w_up, m_w_down, v_wq, v_wk, v_wv, v_wo, v_w_gate, v_w_up, v_w_down):
    weights = dict(zip(NAMES, (wq, wk, wv, wo, w_gate, w_up, w_down), strict=True))

    def take(so_far, sequence):
        h, by_y = sequence
        _, back = jax.vjp(stack, weights, h)
        by_weights, by_h = back(by_y)
        return jax.tree.map(lambda total, term: total + term.astype(jnp.float32), so_far, by_weights), by_h

    none_yet = {name: jnp.zeros(w.shape, jnp.float32) for name, w in weights.items()}
    by_weights, by_x = lax.scan(take, none_yet, (x, dy))
    gradients = [by_weights[name].astype(jnp.bfloat16).astype(jnp.float32) for name in NAMES]
    gradients = clipped(gradients, sum(jnp.sum(g * g) for g in gradients), sum(g.size for g in gradients))
    first = (m_wq, m_wk, m_wv, m_wo, m_w_gate, m_w_up, m_w_down)
    second = (v_wq, v_wk, v_wv, v_wo, v_w_gate, v_w_up, v_w_down)
    new = [adamw(weights[name].astype(jnp.float32), m, v, g) for name, m, v, g in zip(NAMES, first, second, gradients, strict=True)]
    return tuple(one[which] for which in range(3) for one in new)
```

```python
import functools
import math

import jax
import jax.numpy as jnp
from jax import lax
from jax.experimental import pallas as pl
from jax.experimental.pallas import tpu as pltpu
from jax.sharding import PartitionSpec as P

HEAD, THETA = 128, 10000
NEG = -1e30
HIDDEN = 2 * NEG
LOG2E = 1.4426950408889634
VMEM = 60 * 2**20
TILE, WIDTH = 256, 512
LOW, WIDE = jnp.bfloat16, jnp.float32
ALL = slice(None)
COST = 10**9
ANY = pl.BlockSpec(memory_space=pl.ANY)
ONCHIP = pl.BlockSpec(memory_space=pltpu.VMEM)
MESH = pl.DeviceIdType.MESH


def _dot(a, b, ca, cb):
    return lax.dot_general(a, b, (((ca,), (cb,)), ((), ())), preferred_element_type=WIDE)


def _nn(a, b):
    return _dot(a, b, 1, 0)


def _nt(a, b):
    return _dot(a, b, 1, 1)


def _tn(a, b):
    return _dot(a, b, 0, 0)


def _low(a):
    return a.astype(LOW)


def _sds(shape, dtype=LOW):
    return jax.ShapeDtypeStruct(shape, dtype)


def _spec(shape, **index):
    return pl.BlockSpec(shape, lambda *g: tuple(index[f"a{k}"](*g) if f"a{k}" in index else 0 for k in range(len(shape))))


def _first(i, *_):
    return i


def _loop(a, b, body):
    lax.fori_loop(a, b, lambda i, _: body(i), None)


def _split(refs, *counts):
    groups = []
    for n in counts:
        groups.append(refs[:n])
        refs = refs[n:]
    return (*groups, refs)


def _call(kernel, name, grid, ins, outs, shapes, scratch, flops, args, aliases=None, talks=None):
    nbytes = sum(math.prod(a.shape) * a.dtype.itemsize for a in (*args, *shapes))
    params = dict(vmem_limit_bytes=VMEM, dimension_semantics=("arbitrary",) * len(grid))
    if talks is not None:
        params.update(collective_id=talks, has_side_effects=True)
    return pl.pallas_call(
        kernel,
        grid_spec=pl.GridSpec(grid=grid, in_specs=ins, out_specs=outs, scratch_shapes=scratch),
        out_shape=shapes,
        compiler_params=pltpu.CompilerParams(**params),
        cost_estimate=pl.CostEstimate(flops=flops, transcendentals=0, bytes_accessed=nbytes),
        input_output_aliases=aliases or {},
        name=name,
    )(*args)


def _pile(acc, i, part):
    @pl.when(i == 0)
    def _():
        acc[:] = part

    @pl.when(i > 0)
    def _():
        acc[:] += part


def _scale(wide):
    return lax.rsqrt(jnp.mean(wide**2, -1, keepdims=True) + 1e-6)


def _normed(h):
    wide = h.astype(WIDE)
    return _low(wide * _scale(wide))


def _norm_back(h, d):
    wide, d = h.astype(WIDE), d.astype(WIDE)
    scale = _scale(wide)
    inner = jnp.mean(d * wide, -1, keepdims=True)
    return _low(d * scale - wide * (scale * scale * scale * inner))


def _swap(one):
    return pltpu.roll(one, HEAD // 2, 1)


def _heads(n):
    return [slice(i * HEAD, i * HEAD + HEAD) for i in range(n)]


def qkv_forward(h, w, cos, sin):
    t, d = h.shape
    width = w.shape[1]
    wide = 2 * WIDTH
    n = width // wide

    def kernel(h_ref, w_ref, cos_ref, sin_ref, o_ref, a_s):
        i = pl.program_id(0)

        @pl.when(i == 0)
        def _():
            a_s[:] = _normed(h_ref[:])

        def run(turn):
            for k in range(0, wide, TILE):
                y = _low(_nn(a_s[:], w_ref[:, k : k + TILE]))
                if turn:
                    y = y.astype(WIDE)
                    y = _low(jnp.concatenate([y[:, c] * cos_ref[:] + _swap(y[:, c]) * sin_ref[:] for c in _heads(TILE // HEAD)], axis=1))
                o_ref[:, k : k + TILE] = y

        pl.when(i < n - n // 3)(lambda: run(True))
        pl.when(i >= n - n // 3)(lambda: run(False))

    angle = _spec((t, HEAD))
    return _call(kernel, "qkv", (n,), [_spec((t, d)), _spec((d, wide), a1=_first), angle, angle], [_spec((t, wide), a1=_first)],
                 [_sds((t, width))], [pltpu.VMEM((t, d), LOW)], 2 * t * d * width, [h, w, cos, sin])[0]


def attend(qkv, heads, beside=None):
    t, f = qkv.shape[0], heads * HEAD
    bq = bk = TILE
    group, extra = 4, 8
    scale = HEAD**-0.5
    e = scale * LOG2E

    other, n = Beside(beside), t // bq

    def kernel(q_ref, k_ref, v_ref, *rest):
        (o_ref, ot_ref, lse_ref, top_s, mix_s), job = other.split(rest, 0, 3)
        iq = pl.program_id(0)
        job.before(iq, n - 1)
        top_s[:] = jnp.full(top_s.shape, NEG, WIDE)
        mix_s[:] = jnp.zeros(mix_s.shape, WIDE)
        ones = jnp.ones((extra, bk), LOW)
        cols = _heads(heads)

        def block(j, masked):
            here = pl.ds(pl.multiple_of(j * bk, bk), bk)
            scores = [_nt(k_ref[here, c], q_ref[:, c]) for c in cols]
            weights, keeps = [], []
            for i, s in enumerate(scores):
                if masked:
                    ok = lax.broadcasted_iota(jnp.int32, (bk, bq), 1) >= lax.broadcasted_iota(jnp.int32, (bk, bq), 0)
                    s = jnp.where(ok, s, HIDDEN)
                old = top_s[i : i + 1, :]
                top = jnp.maximum(old, s.max(axis=0, keepdims=True))
                top_s[pl.ds(i, 1), :] = top
                weights.append(_low(jnp.exp2((s - top) * e)))
                keeps.append(jnp.exp2((old - top) * e))
            for i, (p, keep) in enumerate(zip(weights, keeps)):
                values = jnp.concatenate([v_ref[here, cols[i]].T, ones], axis=0)
                mix_s[i] = mix_s[i] * keep + _nn(values, p)

        _loop(0, iq, lambda j: block(j, False))
        block(iq, True)
        for i, c in enumerate(cols):
            total = mix_s[i, HEAD : HEAD + 1, :]
            out = _low(mix_s[i, :HEAD, :] * (1 / total))
            ot_ref[c, :] = out
            o_ref[:, c] = out.T
            lse_ref[i // group, i % group : i % group + 1, :] = top_s[i : i + 1, :] * scale + jnp.log(total)
        job.after(iq, n - 1)

    keys = [_spec((t, f), a1=functools.partial(lambda g, i: g, g)) for g in (1, 2)]
    return _call(kernel, "attend", (n,), [_spec((bq, f), a0=_first), *keys, *other.ins],
                 [_spec((bq, f), a0=_first), _spec((f, bq), a1=_first), _spec((heads // group, group, bq), a2=_first), *other.outs],
                 [_sds((t, f)), _sds((f, t)), _sds((heads // group, group, t), WIDE), *other.shapes],
                 [pltpu.VMEM((heads, bq), WIDE), pltpu.VMEM((heads, HEAD + extra, bq), WIDE), *other.scratch], 4 * t * t * f, [qkv] * 3 + other.args, talks=other.talks)


def attend_back(qkv, dot, lse, delta, cos, sin, heads, beside=None):
    t, f = qkv.shape[0], heads * HEAD
    kb, bq, bk = lse.shape[1], WIDTH, TILE
    scale = HEAD**-0.5
    e = scale * LOG2E
    w = kb * HEAD
    nh, nq = heads // kb, t // bq
    other = Beside(beside)

    def kernel(q_ref, k_ref, v_ref, dot_ref, lse_ref, delta_ref, cos_ref, sin_ref, *rest):
        (dq_ref, dk_ref, dv_ref, dq_s, dk_s, dv_s), job = other.split(rest, 0, 3)
        iq = pl.program_id(1)
        step, last = pl.program_id(0) * nq + iq, nh * nq - 1
        job.before(step, last)
        cols = _heads(kb)

        @pl.when(iq == 0)
        def _():
            dk_s[:] = jnp.zeros_like(dk_s)
            dv_s[:] = jnp.zeros_like(dv_s)

        dq_s[:] = jnp.zeros_like(dq_s)
        lses = [lse_ref[0, i : i + 1, :] * LOG2E for i in range(kb)]
        deltas = [delta_ref[0, i : i + 1, :] for i in range(kb)]

        def block(j, masked):
            here = pl.ds(pl.multiple_of(j * bk, bk), bk)
            scores = [_nt(k_ref[here, c], q_ref[:, c]) for c in cols]
            dps = [_nn(v_ref[here, c], dot_ref[c, :]) for c in cols]
            for i, c in enumerate(cols):
                p = jnp.exp2(scores[i] * e - lses[i])
                if masked:
                    ok = (lax.broadcasted_iota(jnp.int32, (bk, bq), 1) + iq * bq) >= (lax.broadcasted_iota(jnp.int32, (bk, bq), 0) + j * bk)
                    p = jnp.where(ok, p, 0.0)
                ds = _low(p * (dps[i] - deltas[i]))
                dv_s[here, c] += _nt(_low(p), dot_ref[c, :])
                dk_s[here, c] += _nn(ds, q_ref[:, c])
                dq_s[i] += _nn(k_ref[here, c].T, ds)

        per = bq // bk
        _loop(0, iq * per, lambda j: block(j, False))
        _loop(iq * per, iq * per + per, lambda j: block(j, True))

        def back(g, at):
            g = _low(g * scale).astype(WIDE)
            return _low(g * cos_ref[at, :] - _swap(g) * sin_ref[at, :])

        for i, c in enumerate(cols):
            dq_ref[:, c] = back(dq_s[i].T, pl.ds(pl.multiple_of(iq * bq, bq), bq))

        @pl.when(iq == nq - 1)
        def _():
            for c in cols:
                dk_ref[:, c] = back(dk_s[:, c], ALL)
            dv_ref[:] = _low(dv_s[:])

        job.after(step, last)

    head = lambda h, i: h
    query = lambda h, i: i
    stats = _spec((1, kb, bq), a0=head, a2=query)
    keys = [_spec((t, w), a1=functools.partial(lambda g, h, i: g * nh + h, g)) for g in range(3)]
    return _call(kernel, "attend_back", (nh, nq),
                 [_spec((bq, w), a0=query, a1=head), *keys[1:], _spec((w, bq), a0=head, a1=query), stats, stats] + [_spec((t, HEAD))] * 2 + other.ins,
                 [_spec((bq, w), a0=query, a1=head), keys[0], keys[0]] + other.outs, [_sds((t, f))] * 3 + other.shapes,
                 [pltpu.VMEM((kb, HEAD, bq), WIDE), pltpu.VMEM((t, w), WIDE), pltpu.VMEM((t, w), WIDE), *other.scratch],
                 10 * t * t * f, [qkv, qkv, qkv, dot, lse, delta, cos, sin, *other.args], talks=other.talks)


def out_forward(h, out, rows, r):
    t, d = h.shape
    f, n = out.shape[1], rows.shape[0]
    at = rows.shape[1] // r - 1

    def kernel(h_ref, out_ref, w_ref, h_out, b_out):
        h = h_ref[:] + _low(_nn(out_ref[:], w_ref[:].reshape(f, d)))
        h_out[:] = h
        b_out[:] = _normed(h)

    row = _spec((WIDTH, d), a0=_first)
    return _call(kernel, "out", (t // WIDTH,), [row, _spec((WIDTH, f), a0=_first), _spec((n, r, d), a1=lambda i: at)],
                 [row, row], [_sds((t, d))] * 2, [], 2 * t * d * f, [h, out, rows])


def out_back(dh, out_t, rows, r, grads, heads, side):
    t, d = dh.shape
    f = heads * HEAD
    wide, chips = WIDTH, side * side
    n, group = f // wide, wide // HEAD
    at = rows.shape[1] // r - 1

    def kernel(dh_ref, ot_ref, w_ref, _, __, dot_ref, delta_ref, own, par, res_s):
        i = pl.program_id(0)
        d_out = _low(_nt(w_ref[:].reshape(wide, d), dh_ref[:]))
        dot_ref[:] = d_out
        prod = d_out.astype(WIDE) * ot_ref[:].astype(WIDE)
        for k, c in enumerate(_heads(group)):
            delta_ref[0, k : k + 1, :] = jnp.sum(prod[c, :], axis=0, keepdims=True)
        res_s[pl.ds(pl.multiple_of(i * wide, wide), wide), :] = _low(_nn(ot_ref[:], dh_ref[:]))

        @pl.when(i == n - 1)
        def _():
            *_, c = _place()
            rows_of = lambda j, c: res_s[pl.ds(pl.multiple_of((_chip(jnp.int32(j), side) * 2 + c) * r, r), r), :]
            for j in range(chips):
                own[j] = rows_of(j, c)
                par[(j % side) * side + j // side] = rows_of(j, 1 - c)

    block = _spec((wide, t), a0=_first)
    g_spec = _spec((chips, r, d), a1=lambda *_: at)
    return _call(kernel, "out_back", (n,), [_spec((t, d)), block, _spec((wide // r, r, d), a0=_first, a1=lambda *_: at), ANY, ANY],
                 [block, _spec((1, group, t), a0=_first), g_spec, g_spec], [_sds((f, t)), _sds((n, group, t), WIDE)] + [_sds(g.shape) for g in grads],
                 [pltpu.VMEM((f, d), LOW)], 4 * t * d * f, [dh, out_t, rows, *grads], aliases={3: 2, 4: 3})


def mlp_forward(h, b, gu, rows, r, beside=None):
    t, d = h.shape
    ff, wide = rows.shape[0] * r, 2 * WIDTH
    n = ff // wide
    other = Beside(beside)

    def kernel(h_ref, b_ref, g_ref, u_ref, d_ref, *rest):
        (o_ref, acc, act), job = other.split(rest, 0, 1)
        i = pl.program_id(0)
        job.before(i, n - 1)
        for k in range(0, wide, TILE):
            gate, up = _nn(b_ref[:], g_ref[:, k : k + TILE]), _nn(b_ref[:], u_ref[:, k : k + TILE])
            act[:, k : k + TILE] = _low(gate * jax.nn.sigmoid(gate) * up)
        _pile(acc, i, _nn(act[:], d_ref[:].reshape(wide, d)))

        @pl.when(i == n - 1)
        def _():
            o_ref[:] = h_ref[:] + _low(acc[:])

        job.after(i, n - 1)

    whole = _spec((t, d))
    return _call(kernel, "mlp", (n,), [whole, whole, _spec((d, wide), a1=_first), _spec((d, wide), a1=lambda i: n + i), _spec((wide // r, r, d), a0=_first), *other.ins],
                 [whole, *other.outs], [_sds((t, d)), *other.shapes], [pltpu.VMEM((t, d), WIDE), pltpu.VMEM((t, wide), LOW), *other.scratch],
                 6 * t * d * ff, [h, b, gu, gu, rows, *other.args], talks=other.talks)


def mlp_back(h, b, dy, gu, rows, r, side, beside=None):
    t, d = h.shape
    other = Beside(beside)
    chips = side * side
    ff, wide = rows.shape[0] * r, 2 * r
    n = ff // wide

    def kernel(h_ref, b_ref, bt_ref, dy_ref, g_ref, u_ref, d_ref, *rest):
        (dh_ref, gu_out, own, par, acc, act, dgu), job = other.split(rest, 0, 4)
        i = pl.program_id(0)
        job.before(i, n - 1)
        b, dy = b_ref[:], dy_ref[:]
        for k in range(0, wide, TILE):
            gate, up = _nn(b, g_ref[:, k : k + TILE]), _nn(b, u_ref[:, k : k + TILE])
            dact = _low(_nt(dy, d_ref[:].reshape(wide, d)[k : k + TILE, :])).astype(WIDE)
            sig = jax.nn.sigmoid(gate)
            silu = gate * sig
            act[:, k : k + TILE] = _low(silu * up)
            dgu[:, k : k + TILE] = _low(dact * up * (sig + silu * (1 - sig)))
            dgu[:, wide + k : wide + k + TILE] = _low(dact * silu)
        gu_out[:] = _low(_nn(bt_ref[:], dgu[:]))
        res = _low(_tn(act[:], dy))
        *_, core = _place()
        for c in range(2):

            @pl.when(core == c)
            def _():
                own[0] = res[c * r :][:r]
                par[0] = res[(1 - c) * r :][:r]

        _pile(acc, i, _nt(dgu[:, :wide], g_ref[:]) + _nt(dgu[:, wide:], u_ref[:]))

        @pl.when(i == n - 1)
        def _():
            dh_ref[:] = dy_ref[:] + _norm_back(h_ref[:], _low(acc[:]))

        job.after(i, n - 1)

    row, col = _spec((t, d)), _spec((d, t))
    chip = lambda i: _chip(i, side)
    return _call(kernel, "mlp_back", (n,),
                 [row, row, col, row, _spec((d, wide), a1=chip), _spec((d, wide), a1=lambda i: n + chip(i)), _spec((2, r, d), a0=chip)] + other.ins,
                 [row, _spec((d, 2 * wide), a1=chip), _spec((1, r, d), a0=_first), _spec((1, r, d), a0=lambda i: lax.rem(i, side) * side + lax.div(i, side))] + other.outs,
                 [_sds((t, d)), _sds((d, 2 * ff))] + [_sds((chips, rows.shape[1], d))] * 2 + other.shapes,
                 [pltpu.VMEM((t, d), WIDE), pltpu.VMEM((t, wide), LOW), pltpu.VMEM((t, 2 * wide), LOW)] + other.scratch,
                 16 * t * d * ff, [h, b, b.T, dy, gu, gu, rows, *other.args], talks=other.talks)


def qkv_back(h, a_rel, dh, dqkv, w, last, side):
    t, d = h.shape
    f, wide = dqkv[0].shape[1], WIDTH
    n, half, three = f // wide, d // 2, range(3)
    full = (3, half, f)
    other = Beside(last and Exchange([], [Kind(full, 1, 2, 2, n, side)], *last, side))

    def kernel(h_ref, a_ref, dh_ref, *rest):
        i = pl.program_id(0)
        terms, rest = _split(rest, 3)
        if last:
            _, job = other.split(rest, 0, 0)
            job.before(i, n - 1)
            own, par = job.inside(i)
        else:
            ws, (own, par, out_ref, acc) = _split(rest, 3)
        for g in three:
            res = _low(_nn(a_ref[:], terms[g][:]))
            own[g] = res[:half]
            par[g] = res[half:]
        if last:
            job.filled(i)
            job.after(i, n - 1)
            return
        _pile(acc, i, sum(_nt(terms[g][:], ws[g][:]) for g in three))

        @pl.when(i == n - 1)
        def _():
            out_ref[:] = dh_ref[:] + _norm_back(h_ref[:], _low(acc[:]))

    row, col = _spec((t, d)), _spec((t, wide), a1=_first)
    ins, args = [row, _spec((d, t)), row, col, col, col], [h, a_rel, dh, *dqkv]
    if last:
        outs, shapes, scratch = other.outs, other.shapes, other.scratch
    else:
        ins += [_spec((d, wide), a1=functools.partial(lambda g, i: g * n + i, g)) for g in three]
        args += [w] * 3
        outs, shapes, scratch = [_spec((3, half, wide), a2=_first)] * 2 + [row], [_sds(full)] * 2 + [_sds((t, d))], [pltpu.VMEM((t, d), WIDE)]
    return _call(kernel, "qkv_back", (n,), ins, outs, shapes, scratch, 12 * t * d * f, args, talks=other.talks)


def _place():
    me, side = lax.axis_index("dp"), math.isqrt(lax.axis_size("dp") // 2)
    return lax.div(me, 2 * side), lax.rem(lax.div(me, 2), side), lax.rem(me, 2)


def _chip(place, side):
    x, y, c = _place()
    d1, d2 = lax.div(place, side), lax.rem(place, side)
    move = jnp.where(c == 0, d2, d1)
    return lax.rem(x + move, side) * side + lax.rem(y + d1 + d2 - move, side)


def _near(side):
    x, y, c = _place()
    place = lambda x, y, c: (x * side + y) * 2 + c
    near = [place(x, y, 1 - c)]
    for k in range(2):
        for by in (1, side - 1):
            move = jnp.where(c == k, 0, by)
            near.append(place(lax.rem(x + move, side), lax.rem(y + by - move, side), c))
    return near


def _greet(near):
    barrier = pltpu.get_barrier_semaphore()
    for to in near:
        pl.semaphore_signal(barrier, inc=1, device_id={"dp": to}, device_id_type=MESH)
    pl.semaphore_wait(barrier, len(near))


class Kind:
    def __init__(self, shape, places, split, chunk_axis, chunks, side):
        self.places, self.split, self.chunk_axis, self.chunks = places, split, chunk_axis, chunks
        self.chunk = shape[chunk_axis] // chunks
        self.shape = tuple(self.chunk if i == chunk_axis else n for i, n in enumerate(shape))
        self.per = shape[places] // (side * side)
        self.half = self.shape[split] // 2
        self.result = tuple(self.per if i == places else n for i, n in enumerate(shape))

    def buffer(self, places, halves):
        size = list(self.shape)
        size[self.places] = places * self.per
        size[self.split] = halves * self.half
        return tuple(size)

    def at(self, place=0, places=None, half=None):
        index = [ALL] * len(self.shape)
        if half is not None:
            index[self.split] = pl.ds(half * self.half, self.half)
        if places is not None:
            start = place * self.per
            index[self.places] = pl.ds(start if isinstance(start, int) else pl.multiple_of(start, self.per), places * self.per)
        return tuple(index)

    def part(self, c):
        index = [ALL] * len(self.shape)
        index[self.chunk_axis] = pl.ds(c * self.chunk, self.chunk)
        return tuple(index)


class Beside:
    def __init__(self, job):
        self.job, self.talks = job, job and job.talks
        self.args, self.ins, self.outs, self.shapes, self.scratch = job.wants() if job else ([], [], [], [], [])

    def split(self, refs, ins, outs):
        if not self.job:
            return refs, Nothing()
        mine, given, out, results, rest = _split(refs, ins, len(self.args), outs, len(self.outs))
        own, scratch = _split(rest, len(rest) - len(self.scratch))
        return (*mine, *out, *own), self.job.bind(given, results, scratch)


class Nothing:
    def before(self, step, last):
        pass

    after = before


class Steps:
    def before(self, step, last):
        @pl.when(step == 0)
        def _():
            _greet(_near(self.side))
            self.begin()

        for s in range(last + 1):
            if any(s in steps for steps in self.plan):
                pl.when(step == s)(functools.partial(self.slot, s))

    def after(self, step, last):
        @pl.when(step == last)
        def _():
            for s in range(last + 1, 1 + max(max(steps) for steps in self.plan)):
                self.slot(s)
            self.end()

    def slot(self, s):
        for n, steps in enumerate(self.plan):
            for stage, at in enumerate(steps):
                if at == s:
                    self.stage(n, stage)


class Exchange:
    def __init__(self, pairs, kinds, plan, talks, side):
        assert side == 4
        self.pairs, self.kinds, self.plan, self.talks, self.side = pairs, kinds, plan, talks, side
        self.work = [(k, c) for k in range(len(kinds)) for c in range(kinds[k].chunks)]

    def wants(self):
        scratch, side = [], self.side
        for kind in self.kinds:
            sizes = [kind.shape] * 2 + [kind.buffer(places, halves) for places in (side, 1) for halves in (1, 1, 2, 2)] + [kind.shape] * (not self.pairs)
            scratch += [pltpu.VMEM((kind.chunks, *size), LOW) for size in sizes]
        n, args = len(self.work), [a for pair in self.pairs for a in pair]
        scratch += [pltpu.SemaphoreType.DMA((n,))] + [pltpu.SemaphoreType.DMA((n, 9))] * 2
        results = [k.result for k in self.kinds]
        return args, [ANY] * len(args), [_spec(r) for r in results], [_sds(r) for r in results], scratch

    def bind(self, given, outs, scratch):
        return Exchanging(self, given, outs, scratch)


class Exchanging(Steps):
    def __init__(self, job, given, outs, scratch):
        self.job, self.given, self.outs, self.plan, self.side = job, given, outs, job.plan, job.side
        *buffers, self.load_sem, self.send_sem, self.recv_sem = scratch
        per = len(buffers) // len(job.kinds)
        self.buffers = [buffers[k * per : k * per + per] for k in range(len(job.kinds))]

    def begin(self):
        if self.given:
            for n in range(len(self.job.work)):
                self.copy(n, 0).start()
                self.load(n).start()

    def end(self):
        for n in range(len(self.job.work)):
            for event in range(9):
                self.copy(n, event).wait_send()

    def inside(self, c):
        return self.buffers[0][0].at[c], self.buffers[0][-1].at[c]

    def filled(self, c):
        self.copy(c, 0).start()

    def load(self, n):
        k, c = self.job.work[n]
        return pltpu.make_async_copy(self.given[2 * k].at[self.job.kinds[k].part(c)], self.buffers[k][0].at[c], self.load_sem.at[n])

    def copy(self, n, event):
        k, c = self.job.work[n] if self.given else (0, n)
        kind, side = self.job.kinds[k], self.side
        near = _near(side)
        if event == 0:
            src, to = self.given[2 * k + 1].at[kind.part(c)] if self.given else self.inside(c)[1], near[0]
        else:
            axis, what = divmod(event - 1, 4)
            places = 1 if axis else side
            part = [kind.at(2 * places, places, 0), kind.at(2 * places, places, 1), kind.at(places, places), kind.at(3 * places, places)][what]
            src, to = self.buffers[k][0].at[c].at[part], near[1 + 2 * axis + what % 2]
        return pltpu.make_async_remote_copy(src_ref=src, dst_ref=self.buffers[k][event + 1].at[c], send_sem=self.send_sem.at[n, event],
                                            recv_sem=self.recv_sem.at[n, event], device_id={"dp": to}, device_id_type=MESH)

    def stage(self, n, stage):
        k, c = self.job.work[n]
        kind, side = self.job.kinds[k], self.side
        own, far, up1, down1, next1, last1, up2, down2, next2, last2, *_ = (b.at[c] for b in self.buffers[k])

        def total(index, others):
            out = own[index].astype(WIDE) + far[index].astype(WIDE)
            for ref, at in others:
                out += ref[at].astype(WIDE)
            return out

        def ring(axis, place, inner, at):
            first, d2s = 1 + 4 * axis, 1 if axis else side
            up, down = (up2, down2) if axis else (up1, down1)

            def put(which, half, others):
                def one(i):
                    index = kind.at(place(which, i), 1, half)
                    own[index] = _low(total(index, inner(which, half) + [(ref, at(i)) for ref in others]))

                if axis:
                    one(0)
                else:
                    _loop(0, d2s, one)

            if stage == 2 * axis:
                put(2, None, [])
                self.copy(n, first).start()
                self.copy(n, first + 1).start()
            else:
                self.copy(n, first).wait_recv()
                put(1, 0, [up])
                put(1, 1, [])
                self.copy(n, first + 2).start()
                self.copy(n, first + 1).wait_recv()
                put(3, 0, [])
                put(3, 1, [down])
                self.copy(n, first + 3).start()

        both = lambda d2, half: [(ref, kind.at(d2, 1, half)) for ref in (next1, last1)]
        if stage == 0:
            if self.given:
                self.load(n).wait()
            self.copy(n, 0).wait_recv()
        if stage == 2:
            for event in (3, 4):
                self.copy(n, event).wait_recv()
        if stage < 2:
            ring(0, lambda which, i: which * side + i, lambda which, half: [], lambda i: kind.at(i, 1))
        elif stage < 4:
            ring(1, lambda which, i: which, both, lambda i: kind.at())
        else:
            for event in (7, 8):
                self.copy(n, event).wait_recv()
            self.outs[k][kind.part(c)] = _low(total(kind.at(0, 1), both(0, None) + [(next2, kind.at()), (last2, kind.at())]))


class Gather:
    def __init__(self, parts, axis, cut, chunks, number, plan, talks, side):
        self.parts, self.axis, self.cut, self.number, self.plan, self.talks, self.side = parts, axis, cut, number, plan, talks, side
        lengths = [w.shape[1 + axis] for w in parts]
        self.starts = [(sum(lengths[:i]), n) for i, n in enumerate(lengths)]
        self.shard = list(parts[0].shape[1:])
        self.shard[axis] = sum(lengths)
        self.chunk = self.shard[cut] // chunks
        self.table, sides = [], range(side)

        def event(d1, d2, to, half=None):
            self.table.append((d1, d2, to, half))
            return len(self.table) - 1

        core, up1, down1, up2, down2 = range(5)
        last = side - 1
        self.second = [event(0, 0, up2), event(0, 0, down2)]
        self.second_on = [event(0, last, up2, 0), event(0, 1, down2, 1)]
        self.up, self.down = ([event(0, i, to) for i in sides] for to in (up1, down1))
        self.on = [event(last, i, up1) if i < 2 else event(1, i, down1) for i in sides]
        self.core = [[event(i, k, core) for k in sides] for i in sides]

    def wants(self):
        n, events = len(self.plan), len(self.table)
        scratch = [pltpu.VMEM(tuple(self.shard), LOW), pltpu.SemaphoreType.DMA((len(self.parts) + 1,))] + [pltpu.SemaphoreType.DMA((n, events))] * 2
        return list(self.parts), [ANY] * len(self.parts), [ANY], [_sds((self.side, self.side, 2, *self.shard))], scratch

    def bind(self, given, outs, scratch):
        return Gathering(self, given, outs, scratch)


class Gathering(Steps):
    def __init__(self, job, given, outs, scratch):
        self.job, self.given, self.out, self.plan, self.side = job, given, outs[0], job.plan, job.side
        self.own, self.load_sem, self.send_sem, self.recv_sem = scratch

    def cutting(self, axis, start, size):
        return tuple(pl.ds(start, size) if i == axis else ALL for i in range(2))

    def load(self, i):
        job = self.job
        return pltpu.make_async_copy(self.given[i].at[job.number], self.own.at[self.cutting(job.axis, *job.starts[i])], self.load_sem.at[i])

    def shard(self, d1, d2):
        x, y, c = _place()
        move = jnp.where(c == 0, d2, d1)
        return self.out.at[lax.rem(x + move, self.side), lax.rem(y + d1 + d2 - move, self.side), c]

    def keep(self):
        return pltpu.make_async_copy(self.own, self.shard(0, 0), self.load_sem.at[len(self.given)])

    def copy(self, n, event):
        job = self.job
        d1, d2, to, half = job.table[event]
        part = (n * job.chunk, job.chunk) if half is None else (n * job.chunk + half * (job.chunk // 2), job.chunk // 2)
        part = self.cutting(job.cut, *part)
        dst = self.shard(d1, d2).at[part]
        src = self.own.at[part] if d1 == d2 == 0 else dst
        return pltpu.make_async_remote_copy(src_ref=src, dst_ref=dst, send_sem=self.send_sem.at[n, event], recv_sem=self.recv_sem.at[n, event],
                                            device_id={"dp": _near(self.side)[to]}, device_id_type=MESH)

    def begin(self):
        for i in range(len(self.given)):
            self.load(i).start()
        for i in range(len(self.given)):
            self.load(i).wait()
        self.keep().start()

    def end(self):
        for n in range(len(self.plan)):
            for event in range(len(self.job.table)):
                self.copy(n, event).wait_send()
        self.keep().wait()

    def stage(self, n, stage):
        job, side = self.job, self.side
        order = (0, side - 1, 1, 2)

        def start(*events):
            for event in events:
                self.copy(n, event).start()

        def came(event):
            self.copy(n, event).wait_recv()

        def forward(i):
            start(job.up[i], job.down[i], job.core[0][i])

        if stage == 0:
            start(*job.second)
            forward(0)
        elif stage == 1:
            for event, on, i in zip(job.second, job.second_on, order[1:]):
                came(event)
                start(on)
                forward(i)
        elif stage == 2:
            for event in job.second_on:
                came(event)
            forward(2)
        elif stage == 3:
            for i in order:
                for k, (event, d1) in enumerate(((job.up[i], side - 1), (job.down[i], 1))):
                    came(event)
                    start(*([job.on[i]] if (i < 2) == (k == 0) else []), job.core[d1][i])
        elif stage == 4:
            for i in order:
                came(job.on[i])
                start(job.core[2][i])
        else:
            for events in job.core:
                for event in events:
                    came(event)


def alone(job, name):
    other = Beside(job)

    def kernel(*refs):
        _, code = other.split(refs, 0, 0)
        code.before(0, 0)
        code.after(0, 0)

    return _call(kernel, name, (), other.ins, other.outs, other.shapes, other.scratch, COST, other.args, talks=other.talks)[0]


def clip(grads, count, devices, talks):
    block = (8, HEAD)

    def kernel(*refs):
        gs, (out_ref, mine, slots, send_sem, recv_sem) = refs[: len(grads)], refs[len(grads) :]
        me = lax.axis_index("dp")
        barrier = pltpu.get_barrier_semaphore()
        to = lambda k: {"dp": lax.rem(me + k, devices)}
        each = functools.partial(_loop, 1, devices)
        each(lambda k: pl.semaphore_signal(barrier, inc=1, device_id=to(k), device_id_type=MESH))
        mine[:] = jnp.broadcast_to(sum(jnp.sum(g[:].astype(WIDE) ** 2) for g in gs), block)
        pl.semaphore_wait(barrier, devices - 1)

        def copy(k, slot):
            return pltpu.make_async_remote_copy(src_ref=mine, dst_ref=slots.at[slot], send_sem=send_sem.at[k], recv_sem=recv_sem.at[slot],
                                                device_id=to(k), device_id_type=MESH)

        each(lambda k: copy(k, me).start())
        slots[pl.ds(me, 1)] = mine[:][None]
        each(lambda k: copy(k, lax.rem(me + devices - k, devices)).wait_recv())
        each(lambda k: copy(k, me).wait_send())
        out_ref[:] = jnp.minimum(1.0, 0.5 * lax.rsqrt(jnp.sum(slots[:], axis=0) / count + 1e-30))

    return _call(kernel, "clip", (), [ONCHIP] * len(grads), [ONCHIP], [_sds(block, WIDE)],
                 [pltpu.VMEM(block, WIDE), pltpu.VMEM((devices, *block), WIDE)] + [pltpu.SemaphoreType.DMA((devices,))] * 2, COST, grads, talks=talks)[0]


def adamw(factor, weights, ms, vs, grads, chips):
    steps, layers, count = 4, len(grads), len(weights)
    blocks, maps = [], []
    for w in weights:
        l, r, n = w.shape
        tall = r % (steps * 16) == 0
        blocks.append((l, r // steps, n) if tall else (l, r, n // steps))
        maps.append("a1" if tall else "a2")
    specs = [_spec(b, **{m: _first}) for b, m in zip(blocks, maps)]
    rd, ro = blocks[6][1], blocks[3][1]
    g_specs, g_args = [], []
    for qkv, rows, gu in grads:
        d = rows.shape[1]
        after = functools.partial(lambda off, i: off + i, steps * rd // ro)
        g_specs += [_spec((*qkv.shape[:2], qkv.shape[2] // steps), a2=_first), _spec((rd, d), a0=_first), _spec((ro, d), a0=after), _spec((gu.shape[0], gu.shape[1] // steps), a1=_first)]
        g_args += [qkv, rows, rows, gu]

    def kernel(factor_ref, *refs):
        ws, m_refs, v_refs, gs, outs = _split(refs, *[count] * 3, len(g_args))
        factor = factor_ref[:1, :1]
        for l in range(layers):
            (qkv, down, out, gu), gs = gs[:4], gs[4:]
            per = chips // steps
            wide = gu.shape[1] // (2 * per)
            halves = [jnp.concatenate([gu[:, pl.ds((2 * p + k) * wide, wide)] for p in range(per)], axis=1) for k in range(2)]
            for i, g in enumerate((*[qkv[k] for k in range(3)], out[:], *halves, down[:])):
                g = g.astype(WIDE) * factor
                m = 0.9 * m_refs[i][l] + 0.1 * g
                v = 0.95 * v_refs[i][l] + 0.05 * g * g
                w = ws[i][l].astype(WIDE)
                outs[i][l] = _low(w - 0.02 * (m * lax.rsqrt(v + 1e-8) + 0.1 * w))
                outs[count + i][l] = m
                outs[2 * count + i][l] = v

    shapes = [_sds(w.shape, kind) for kind in (LOW, WIDE, WIDE) for w in weights]
    return _call(kernel, "adamw", (steps,), [_spec(factor.shape)] + specs * 3 + g_specs, specs * 3, shapes, [], COST, [factor, *weights, *ms, *vs, *g_args])


def solution(mesh):
    devices = mesh.shape["dp"]
    side = math.isqrt(devices // 2)
    chips = side * side

    def step(x, dy, *arrays):
        weights, ms, vs, _ = _split(arrays, *[len(arrays) // 3] * 3)
        wq, wk, wv, wo, wg, wu, wd = weights
        layers = wq.shape[0]
        x, dy = x[0], dy[0]
        t, d = x.shape
        f, ff = wq.shape[2], wg.shape[2]
        heads = f // HEAD
        rd, ro = wd.shape[1], wo.shape[1]
        *_, c = _place()
        chip = _chip(jnp.arange(chips, dtype=jnp.int32), side)
        other = chip.reshape(side, side).T.reshape(-1)
        per = d // devices
        rel = jnp.concatenate([chip * 2 + c, other * 2 + 1 - c])
        rel = (rel[:, None] * per + jnp.arange(per, dtype=jnp.int32)).reshape(-1)
        onehot = _low(jnp.arange(d, dtype=jnp.int32)[:, None] == rel)
        relative = lambda a: _low(_dot(onehot, a, 0, 1))
        half = HEAD // 2
        angle = jnp.arange(t, dtype=WIDE)[:, None] * THETA ** (-jnp.arange(half, dtype=WIDE) / half)
        cos = jnp.concatenate([jnp.cos(angle)] * 2, 1)
        sin = jnp.concatenate([-jnp.sin(angle), jnp.sin(angle)], 1)
        gather = lambda ws, n: lax.all_gather(jnp.concatenate([w[n] for w in ws], 1), "dp", axis=0, tiled=True)
        rows_job = lambda n: Gather((wd, wo), 0, 0, 2, n, [list(range(k, k + 6)) for k in range(2)], 6 + n, side)
        w_qkv = [alone(Gather((wq, wk, wv), 1, 1, 2, 0, [[s + n for s in range(1, 7)] for n in range(2)], 1, side), "gathered").reshape(d, -1)]
        w_gu = [gather((wg, wu), 0)]
        w_qkv += [gather((wq, wk, wv), 1)]
        w_gu += [gather((wg, wu), 1)]
        h, kept = x, []
        job = rows_job(0)
        for n in range(layers):
            qkv = qkv_forward(h, w_qkv[n], cos, sin)
            out, out_t, lse, *more = attend(qkv, heads, job)
            if job:
                rows, job = [more[0].reshape(devices, -1, d)], None
            h2, b = out_forward(h, out, rows[n], ro)
            kept.append((h, qkv, out_t, lse, h2, b))
            if n < layers - 1:
                h, more = mlp_forward(h2, b, w_gu[n], rows[n], rd, rows_job(1))
                rows.append(more.reshape(devices, -1, d))
        g_gu, g_rows, g_qkv = ([None] * layers for _ in range(3))
        scatter = lambda a: lax.psum_scatter(a, "dp", scatter_dimension=0, tiled=True)
        dh, job = dy, None
        rows_kind = lambda pair: Kind(pair[0].shape, 0, 1, 1, 2, side)
        for n in reversed(range(layers)):
            h, qkv, out_t, lse, h2, b = kept[n]
            dh2, gu, *pair, = mlp_back(h2, b, dh, w_gu[n], rows[n], rd, side, job)
            if job:
                pair, (g_rows[n + 1], g_qkv[n + 1]) = pair[:2], pair[2:]
            dot, delta, *pair = out_back(dh2, out_t, rows[n], ro, pair, heads, side)
            job = None
            if n == 0:
                dot, g_gu[1] = lax.optimization_barrier((dot, g_gu[1]))
                job = Exchange([pair], [rows_kind(pair)], [[1, 2, 4, 5, 6], [2, 4, *range(6, 9)]], 2, side)
            g_gu[n] = scatter(gu)
            *dqkv, = attend_back(qkv, dot, lse, delta, cos, sin, heads, job)
            a_rel = relative(_normed(h))
            if n == 0:
                g_rows[0] = dqkv.pop()
                g_qkv[0] = qkv_back(h, a_rel, dh2, dqkv, w_qkv[n], ([[1 + s + g for s in range(5)] for g in range(4)], 4), side)[0]
            else:
                *two, dh = qkv_back(h, a_rel, dh2, dqkv, w_qkv[n], None, side)
                job = Exchange([pair, two], [rows_kind(pair), Kind(two[0].shape, 1, 2, 2, 2, side)], [[first + 2 * s for s in range(5)] for first in (1, 2, 5, 6)], 3, side)
        grads = [(g_qkv[n], g_rows[n][0], g_gu[n]) for n in range(layers)]
        factor = clip([g for one in grads for g in one], sum(w.size for w in weights) * devices, devices, 5)
        return tuple(adamw(factor, weights, ms, vs, grads, chips))

    states, cut = P(("rep", "dp"), None, None), P(None, "dp", None)
    return jax.shard_map(step, mesh=mesh, in_specs=(states, states) + (cut,) * 21, out_specs=(P("rep", "dp", None),) * 21, check_vma=False)
```

```python
import functools
import math

import jax
import jax.numpy as jnp
from jax import lax
from jax.experimental import pallas as pl
from jax.experimental.pallas import tpu as pltpu
from jax.sharding import PartitionSpec as P

HEAD, THETA = 128, 10000
NEG = -1e30
HIDDEN = 2 * NEG
LOG2E = 1.4426950408889634
VMEM = 62 * 2**20
TILE, WIDTH = 256, 512
LOW, WIDE = jnp.bfloat16, jnp.float32
ALL = slice(None)
COST = 10**9
ANY = pl.BlockSpec(memory_space=pl.ANY)
ONCHIP = pl.BlockSpec(memory_space=pltpu.VMEM)
MESH = pl.DeviceIdType.MESH


def _dot(a, b, ca, cb):
    return lax.dot_general(a, b, (((ca,), (cb,)), ((), ())), preferred_element_type=WIDE)


def _nn(a, b):
    return _dot(a, b, 1, 0)


def _nt(a, b):
    return _dot(a, b, 1, 1)


def _tn(a, b):
    return _dot(a, b, 0, 0)


def _low(a):
    return a.astype(LOW)


def _sds(shape, dtype=LOW):
    return jax.ShapeDtypeStruct(shape, dtype)


def _spec(shape, **index):
    return pl.BlockSpec(shape, lambda *g: tuple(index[f"a{k}"](*g) if f"a{k}" in index else 0 for k in range(len(shape))))


def _first(i, *_):
    return i


def _loop(a, b, body):
    lax.fori_loop(a, b, lambda i, _: body(i), None)


def _split(refs, *counts):
    groups = []
    for n in counts:
        groups.append(refs[:n])
        refs = refs[n:]
    return (*groups, refs)


def _call(kernel, name, grid, ins, outs, shapes, scratch, flops, args, aliases=None, talks=None):
    nbytes = sum(math.prod(a.shape) * a.dtype.itemsize for a in (*args, *shapes))
    params = dict(vmem_limit_bytes=VMEM, dimension_semantics=("arbitrary",) * len(grid))
    if talks is not None:
        params.update(collective_id=talks, has_side_effects=True)
    return pl.pallas_call(
        kernel,
        grid_spec=pl.GridSpec(grid=grid, in_specs=ins, out_specs=outs, scratch_shapes=scratch),
        out_shape=shapes,
        compiler_params=pltpu.CompilerParams(**params),
        cost_estimate=pl.CostEstimate(flops=flops, transcendentals=0, bytes_accessed=nbytes),
        input_output_aliases=aliases or {},
        name=name,
    )(*args)


def _clear(acc, i):
    @pl.when(i == 0)
    def _():
        acc[:] = jnp.zeros_like(acc)


def _scale(wide):
    return lax.rsqrt(jnp.mean(wide**2, -1, keepdims=True) + 1e-6)


def _normed(h):
    wide = h.astype(WIDE)
    return _low(wide * _scale(wide))


def _norm_back(h, d):
    wide, d = h.astype(WIDE), d.astype(WIDE)
    scale = _scale(wide)
    inner = jnp.mean(d * wide, -1, keepdims=True)
    return _low(d * scale - wide * (scale * scale * scale * inner))


def _swap(one):
    return pltpu.roll(one, HEAD // 2, 1)


def _heads(n):
    return [slice(i * HEAD, i * HEAD + HEAD) for i in range(n)]


def qkv_forward(h, w, cos, sin):
    t, d = h.shape
    width = w.shape[1]
    wide = 2 * WIDTH
    n = width // wide

    def kernel(h_ref, w_ref, cos_ref, sin_ref, o_ref, a_s):
        i = pl.program_id(0)

        @pl.when(i == 0)
        def _():
            a_s[:] = _normed(h_ref[:])

        def run(turn):
            for k in range(0, wide, TILE):
                y = _low(_nn(a_s[:], w_ref[:, k : k + TILE]))
                if turn:
                    y = y.astype(WIDE)
                    y = _low(jnp.concatenate([y[:, c] * cos_ref[:] + _swap(y[:, c]) * sin_ref[:] for c in _heads(TILE // HEAD)], axis=1))
                o_ref[:, k : k + TILE] = y

        pl.when(i < n - n // 3)(lambda: run(True))
        pl.when(i >= n - n // 3)(lambda: run(False))

    angle = _spec((t, HEAD))
    return _call(kernel, "qkv", (n,), [_spec((t, d)), _spec((d, wide), a1=_first), angle, angle], [_spec((t, wide), a1=_first)],
                 [_sds((t, width))], [pltpu.VMEM((t, d), LOW)], 2 * t * d * width, [h, w, cos, sin])[0]


def attend(qkv, heads, beside=None):
    t, f = qkv.shape[0], heads * HEAD
    bq = bk = TILE
    group = extra = 8
    scale = HEAD**-0.5
    e = scale * LOG2E

    other, n = Beside(beside), t // bq

    def kernel(q_ref, k_ref, v_ref, *rest):
        (o_ref, ot_ref, lse_ref, top_s, mix_s), job = other.split(rest, 0, 3)
        iq = pl.program_id(0)
        job.before(2 * iq, 2 * n - 1, False)
        top_s[:] = jnp.full(top_s.shape, NEG, WIDE)
        mix_s[:] = jnp.zeros(mix_s.shape, WIDE)
        ones = jnp.ones((extra, bk), LOW)
        cols = _heads(heads)

        def block(j, masked):
            here = pl.ds(pl.multiple_of(j * bk, bk), bk)
            scores = [_nt(k_ref[here, c], q_ref[:, c]) for c in cols]
            weights, keeps = [], []
            for i, s in enumerate(scores):
                if masked:
                    ok = lax.broadcasted_iota(jnp.int32, (bk, bq), 1) >= lax.broadcasted_iota(jnp.int32, (bk, bq), 0)
                    s = jnp.where(ok, s, HIDDEN)
                old = top_s[i : i + 1, :]
                top = jnp.maximum(old, s.max(axis=0, keepdims=True))
                top_s[pl.ds(i, 1), :] = top
                weights.append(_low(jnp.exp2((s - top) * e)))
                keeps.append(jnp.exp2((old - top) * e))
            for i, (p, keep) in enumerate(zip(weights, keeps)):
                values = jnp.concatenate([v_ref[here, cols[i]].T, ones], axis=0)
                mix_s[i] = mix_s[i] * keep + _nn(values, p)

        _loop(0, iq, lambda j: block(j, False))
        job.before(2 * iq + 1, 2 * n - 1, True)
        block(iq, True)
        for i, c in enumerate(cols):
            total = mix_s[i, HEAD : HEAD + 1, :]
            out = _low(mix_s[i, :HEAD, :] * (1 / total))
            ot_ref[c, :] = out
            o_ref[:, c] = out.T
            lse_ref[i // group, i % group : i % group + 1, :] = top_s[i : i + 1, :] * scale + jnp.log(total)
        job.after(2 * iq + 1, 2 * n - 1)

    keys = [_spec((t, f), a1=functools.partial(lambda g, i: g, g)) for g in (1, 2)]
    return _call(kernel, "attend", (n,), [_spec((bq, f), a0=_first), *keys, *other.ins],
                 [_spec((bq, f), a0=_first), _spec((f, bq), a1=_first), _spec((heads // group, group, bq), a2=_first), *other.outs],
                 [_sds((t, f)), _sds((f, t)), _sds((heads // group, group, t), WIDE), *other.shapes],
                 [pltpu.VMEM((heads, bq), WIDE), pltpu.VMEM((heads, HEAD + extra, bq), WIDE), *other.scratch], 4 * t * t * f, [qkv] * 3 + other.args, talks=other.talks)


def attend_back(qkv, dot, lse, delta, cos, sin, heads, beside=None):
    t, f = qkv.shape[0], heads * HEAD
    kb, bq, bk = lse.shape[1], TILE, TILE
    scale = HEAD**-0.5
    e = scale * LOG2E
    w = kb * HEAD
    nh, nq = heads // kb, t // bq
    other = Beside(beside)

    def kernel(q_ref, k_ref, v_ref, dot_ref, lse_ref, delta_ref, cos_ref, sin_ref, *rest):
        (dq_ref, dk_ref, dv_ref, dq_s, dk_s, dv_s), job = other.split(rest, 0, 3)
        iq = pl.program_id(1)
        step, last = 2 * (pl.program_id(0) * nq + iq), 2 * nh * nq - 1
        job.before(step, last, False)
        cols = _heads(kb)

        @pl.when(iq == 0)
        def _():
            dk_s[:] = jnp.zeros_like(dk_s)
            dv_s[:] = jnp.zeros_like(dv_s)

        dq_s[:] = jnp.zeros_like(dq_s)
        lses = [lse_ref[0, i : i + 1, :] * LOG2E for i in range(kb)]
        deltas = [delta_ref[0, i : i + 1, :] for i in range(kb)]

        def block(j, masked):
            here = pl.ds(pl.multiple_of(j * bk, bk), bk)
            scores = [_nt(k_ref[here, c], q_ref[:, c]) for c in cols]
            dps = [_nn(v_ref[here, c], dot_ref[c, :]) for c in cols]
            for i, c in enumerate(cols):
                p = jnp.exp2(scores[i] * e - lses[i])
                if masked:
                    ok = (lax.broadcasted_iota(jnp.int32, (bk, bq), 1) + iq * bq) >= (lax.broadcasted_iota(jnp.int32, (bk, bq), 0) + j * bk)
                    p = jnp.where(ok, p, 0.0)
                ds = _low(p * (dps[i] - deltas[i]))
                dv_s[here, c] += _nt(_low(p), dot_ref[c, :])
                dk_s[here, c] += _nn(ds, q_ref[:, c])
                dq_s[i] += _nn(k_ref[here, c].T, ds)

        per = bq // bk
        _loop(0, iq * per, lambda j: block(j, False))
        job.before(step + 1, last, True)
        _loop(iq * per, iq * per + per, lambda j: block(j, True))

        def back(g, at):
            g = _low(g * scale).astype(WIDE)
            return _low(g * cos_ref[at, :] - _swap(g) * sin_ref[at, :])

        for i, c in enumerate(cols):
            dq_ref[:, c] = back(dq_s[i].T, pl.ds(pl.multiple_of(iq * bq, bq), bq))

        @pl.when(iq == nq - 1)
        def _():
            for c in cols:
                dk_ref[:, c] = back(dk_s[:, c], ALL)
            dv_ref[:] = _low(dv_s[:])

        job.after(step + 1, last)

    head = lambda h, i: h
    query = lambda h, i: i
    stats = _spec((1, kb, bq), a0=head, a2=query)
    keys = [_spec((t, w), a1=functools.partial(lambda g, h, i: g * nh + h, g)) for g in range(3)]
    return _call(kernel, "attend_back", (nh, nq),
                 [_spec((bq, w), a0=query, a1=head), *keys[1:], _spec((w, bq), a0=head, a1=query), stats, stats] + [_spec((t, HEAD))] * 2 + other.ins,
                 [_spec((bq, w), a0=query, a1=head), keys[0], keys[0]] + other.outs, [_sds((t, f))] * 3 + other.shapes,
                 [pltpu.VMEM((kb, HEAD, bq), WIDE), pltpu.VMEM((t, w), WIDE), pltpu.VMEM((t, w), WIDE), *other.scratch],
                 10 * t * t * f, [qkv, qkv, qkv, dot, lse, delta, cos, sin, *other.args], talks=other.talks)


def out_forward(h, out, rows, r):
    t, d = h.shape
    f, n = out.shape[1], rows.shape[0]
    at = rows.shape[1] // r - 1

    def kernel(h_ref, out_ref, w_ref, h_out, b_out, bt_out):
        h = h_ref[:] + _low(_nn(out_ref[:], w_ref[:].reshape(f, d)))
        h_out[:] = h
        b = _normed(h)
        b_out[:] = b
        bt_out[:] = b.T

    row = _spec((WIDTH, d), a0=_first)
    return _call(kernel, "out", (t // WIDTH,), [row, _spec((WIDTH, f), a0=_first), _spec((n, r, d), a1=lambda i: at)],
                 [row, row, _spec((d, WIDTH), a1=_first)], [_sds((t, d))] * 2 + [_sds((d, t))], [], 2 * t * d * f, [h, out, rows])


def out_back(dh, out_t, rows, r, grads, heads, side):
    t, d = dh.shape
    f = heads * HEAD
    wide, chips = 2 * WIDTH, side * side
    n, group, m = f // wide, wide // HEAD, len(grads)
    at = rows.shape[1] // r - 1

    def kernel(dh_ref, ot_ref, w_ref, *rest):
        _, (dot_ref, delta_ref), outs, (res_s,) = _split(rest, m, 2, m)
        i = pl.program_id(0)
        d_out = _low(_nt(w_ref[:].reshape(wide, d), dh_ref[:]))
        dot_ref[:] = d_out
        prod = d_out.astype(WIDE) * ot_ref[:].astype(WIDE)
        for k, c in enumerate(_heads(group)):
            delta_ref[0, k : k + 1, :] = jnp.sum(prod[c, :], axis=0, keepdims=True)
        res_s[pl.ds(pl.multiple_of(i * wide, wide), wide), :] = _low(_nn(ot_ref[:], dh_ref[:]))

        @pl.when(i == n - 1)
        def _():
            *_, c = _place()
            rows_of = lambda j, c: res_s[pl.ds(pl.multiple_of((_chip(jnp.int32(j), side) * 2 + c) * r, r), r), :]
            for j in range(chips):
                outs[0][j] = rows_of(j, c)
                outs[1][(j % side) * side + j // side] = rows_of(j, 1 - c)

    block = _spec((wide, t), a0=_first)
    w_spec = _spec((wide // r, r, d), a0=_first, a1=lambda *_: at)
    return _call(kernel, "out_back", (n,), [_spec((t, d)), block, w_spec] + [ANY] * m,
                 [block, _spec((1, group, t), a0=_first)] + [_spec((chips, r, d), a1=lambda *_: at)] * m,
                 [_sds((f, t)), _sds((n, group, t), WIDE)] + [_sds(g.shape) for g in grads],
                 [pltpu.VMEM((f, d), LOW)], 4 * t * d * f, [dh, out_t, rows, *grads], aliases={3 + k: 2 + k for k in range(m)})


def mlp_forward(h, b, gu, rows, r, beside=None):
    t, d = h.shape
    ff, wide = rows.shape[0] * r, 2 * WIDTH
    n = ff // wide
    other = Beside(beside)

    def kernel(h_ref, b_ref, g_ref, u_ref, d_ref, *rest):
        (o_ref, acc, act), job = other.split(rest, 0, 1)
        i = pl.program_id(0)
        job.before(i, n - 1)
        _clear(acc, i)
        for k in range(0, wide, TILE):
            gate, up = _nn(b_ref[:], g_ref[:, k : k + TILE]), _nn(b_ref[:], u_ref[:, k : k + TILE])
            act[:, k : k + TILE] = _low(gate * jax.nn.sigmoid(gate) * up)
        acc[:] += _nn(act[:], d_ref[:].reshape(wide, d))

        @pl.when(i == n - 1)
        def _():
            o_ref[:] = h_ref[:] + _low(acc[:])

        job.after(i, n - 1)

    whole = _spec((t, d))
    return _call(kernel, "mlp", (n,), [whole, whole, _spec((d, wide), a1=_first), _spec((d, wide), a1=lambda i: n + i), _spec((wide // r, r, d), a0=_first), *other.ins],
                 [whole, *other.outs], [_sds((t, d)), *other.shapes], [pltpu.VMEM((t, d), WIDE), pltpu.VMEM((t, wide), LOW), *other.scratch],
                 6 * t * d * ff, [h, b, gu, gu, rows, *other.args], talks=other.talks)


def mlp_back(h, b, b_t, dy, gu, rows, r, side, beside=None):
    t, d = h.shape
    wide, n, deep = 2 * r, rows.shape[0] // 2, rows.shape[1]
    other = Beside(beside)

    def kernel(h_ref, b_ref, bt_ref, dy_ref, g_ref, u_ref, d_ref, *rest):
        (dh_ref, gu_out, *d_out, acc, act, dgu, res), job = other.split(rest, 0, 4)
        i = pl.program_id(0)
        job.before(i, n - 1)
        _clear(acc, i)
        b, dy = b_ref[:], dy_ref[:]
        for k in range(0, wide, TILE):
            gate, up = _nn(b, g_ref[:, k : k + TILE]), _nn(b, u_ref[:, k : k + TILE])
            dact = _low(_nt(dy, d_ref[:].reshape(wide, d)[k : k + TILE, :])).astype(WIDE)
            sig = jax.nn.sigmoid(gate)
            silu = gate * sig
            act[:, k : k + TILE] = _low(silu * up)
            dgu[:, k : k + TILE] = _low(dact * up * (sig + silu * (1 - sig)))
            dgu[:, wide + k : wide + k + TILE] = _low(dact * silu)
        gu_out[:] = _low(_nn(bt_ref[:], dgu[:]))
        acc[:] += _nt(dgu[:, :wide], g_ref[:]) + _nt(dgu[:, wide:], u_ref[:])
        res[:] = _low(_tn(act[:], dy))
        *_, core = _place()
        for k, ref in enumerate(d_out):
            ref[0] = res[pl.ds(pl.multiple_of(jnp.where(core == k, 0, r), r), r), :]

        @pl.when(i == n - 1)
        def _():
            dh_ref[:] = dy_ref[:] + _norm_back(h_ref[:], _low(acc[:]))

        job.after(i, n - 1)

    row, col = _spec((t, d)), _spec((d, t))
    d_specs = [_spec((1, r, d), a0=functools.partial(lambda k, i: _back(i, side)[k], k)) for k in range(2)]
    return _call(kernel, "mlp_back", (n,),
                 [row, row, col, row, _spec((d, wide), a1=_first), _spec((d, wide), a1=lambda i: n + i), _spec((2, r, d), a0=_first)] + other.ins,
                 [row, _spec((d, 2 * wide), a1=_first)] + d_specs + other.outs, [_sds((t, d)), _sds((d, 2 * wide * n))] + [_sds((n, deep, d))] * 2 + other.shapes,
                 [pltpu.VMEM((t, d), WIDE), pltpu.VMEM((t, wide), LOW), pltpu.VMEM((t, 2 * wide), LOW), pltpu.VMEM((wide, d), LOW)] + other.scratch,
                 16 * t * d * wide * n, [h, b, b_t, dy, gu, gu, rows, *other.args], talks=other.talks)


def qkv_back(h, a_rel, dh, dqkv, w, last, side):
    t, d = h.shape
    f, wide = dqkv[0].shape[1], WIDTH
    n, half, three = f // wide, d // 2, range(3)
    full = (3, half, f)
    other = Beside(last and Exchange([], [Kind(full, 1, 2, 2, n, side)], *last, side))

    def kernel(h_ref, a_ref, dh_ref, *rest):
        i = pl.program_id(0)
        terms, rest = _split(rest, 3)
        if last:
            _, job = other.split(rest, 0, 0)
            job.before(i, n - 1)
            own, par = job.inside(i)
        else:
            ws, (own, par, out_ref, acc) = _split(rest, 3)
            _clear(acc, i)
        for g in three:
            res = _low(_nn(a_ref[:], terms[g][:]))
            own[g] = res[:half]
            par[g] = res[half:]
        if last:
            job.filled(i)
            job.after(i, n - 1)
            return
        acc[:] += sum(_nt(terms[g][:], ws[g][:]) for g in three)

        @pl.when(i == n - 1)
        def _():
            out_ref[:] = dh_ref[:] + _norm_back(h_ref[:], _low(acc[:]))

    row, col = _spec((t, d)), _spec((t, wide), a1=_first)
    ins, args = [row, _spec((d, t)), row, col, col, col], [h, a_rel, dh, *dqkv]
    if last:
        outs, shapes, scratch = other.outs, other.shapes, other.scratch
    else:
        ins += [_spec((d, wide), a1=functools.partial(lambda g, i: g * n + i, g)) for g in three]
        args += [w] * 3
        outs, shapes, scratch = [_spec((3, half, wide), a2=_first)] * 2 + [row], [_sds(full)] * 2 + [_sds((t, d))], [pltpu.VMEM((t, d), WIDE)]
    return _call(kernel, "qkv_back", (n,), ins, outs, shapes, scratch, 12 * t * d * f, args, talks=other.talks)


def _place():
    me, side = lax.axis_index("dp"), math.isqrt(lax.axis_size("dp") // 2)
    return lax.div(me, 2 * side), lax.rem(lax.div(me, 2), side), lax.rem(me, 2)


def _chip(place, side):
    x, y, c = _place()
    d1, d2 = lax.div(place, side), lax.rem(place, side)
    move = jnp.where(c == 0, d2, d1)
    return lax.rem(x + move, side) * side + lax.rem(y + d1 + d2 - move, side)


def _back(chip, side):
    x, y, c = _place()
    dx, dy = lax.rem(lax.div(chip, side) + side - x, side), lax.rem(lax.rem(chip, side) + side - y, side)
    along = jnp.where(c == 0, dy, dx)
    across = dx + dy - along
    return along * side + across, across * side + along


def _near(side):
    x, y, c = _place()
    place = lambda x, y, c: (x * side + y) * 2 + c
    near = [place(x, y, 1 - c)]
    for k in range(2):
        for by in (1, side - 1):
            move = jnp.where(c == k, 0, by)
            near.append(place(lax.rem(x + move, side), lax.rem(y + by - move, side), c))
    return near


def _greet(near):
    barrier = pltpu.get_barrier_semaphore()
    for to in near:
        pl.semaphore_signal(barrier, inc=1, device_id={"dp": to}, device_id_type=MESH)
    pl.semaphore_wait(barrier, len(near))


class Kind:
    def __init__(self, shape, places, split, chunk_axis, chunks, side):
        self.places, self.split, self.chunk_axis, self.chunks = places, split, chunk_axis, chunks
        self.chunk = shape[chunk_axis] // chunks
        self.shape = tuple(self.chunk if i == chunk_axis else n for i, n in enumerate(shape))
        self.per = shape[places] // (side * side)
        self.half = self.shape[split] // 2
        self.result = tuple(self.per if i == places else n for i, n in enumerate(shape))

    def buffer(self, places, halves):
        size = list(self.shape)
        size[self.places] = places * self.per
        size[self.split] = halves * self.half
        return tuple(size)

    def at(self, place=0, places=None, half=None):
        index = [ALL] * len(self.shape)
        if half is not None:
            index[self.split] = pl.ds(half * self.half, self.half)
        if places is not None:
            start = place * self.per
            index[self.places] = pl.ds(start if isinstance(start, int) else pl.multiple_of(start, self.per), places * self.per)
        return tuple(index)

    def part(self, c):
        index = [ALL] * len(self.shape)
        index[self.chunk_axis] = pl.ds(c * self.chunk, self.chunk)
        return tuple(index)


class Beside:
    def __init__(self, job):
        self.job, self.talks = job, job and job.talks
        self.args, self.ins, self.outs, self.shapes, self.scratch = job.wants() if job else ([], [], [], [], [])

    def split(self, refs, ins, outs):
        if not self.job:
            return refs, Nothing()
        mine, given, out, results, rest = _split(refs, ins, len(self.args), outs, len(self.outs))
        own, scratch = _split(rest, len(rest) - len(self.scratch))
        return (*mine, *out, *own), self.job.bind(given, results, scratch)


class Nothing:
    def before(self, step, last, amid=None):
        pass

    after = before


def _plan(*chunks):
    return [[int(digit, 36) for digit in steps] for steps in chunks]


class Steps:
    def before(self, step, last, amid=None):
        if not amid:

            @pl.when(step == 0)
            def _():
                self.load()
                _greet(_near(self.side))
                self.begin()

        for s in range(last + 1) if amid is None else range(int(amid), last + 1, 2):
            if any(s in steps for steps in self.plan):
                pl.when(step == s)(functools.partial(self.slot, s))

    def after(self, step, last):
        @pl.when(step == last)
        def _():
            for s in range(last + 1, 1 + max(max(steps) for steps in self.plan)):
                self.slot(s)
            self.end()

    def slot(self, s):
        here = [(stage, n) for n, steps in enumerate(self.plan) for stage, at in enumerate(steps) if at == s]
        for stage, n in sorted(here):
            self.stage(n, stage)


class Jobs:
    def __init__(self, *jobs):
        self.jobs, self.talks = jobs, jobs[0].talks

    def wants(self):
        self.parts = [job.wants() for job in self.jobs]
        return [sum((list(part[k]) for part in self.parts), []) for k in range(5)]

    def bind(self, given, outs, scratch):
        return Several(self, given, outs, scratch)


class Several(Steps):
    def __init__(self, job, given, outs, scratch):
        self.side, self.codes = job.jobs[0].side, []
        for one, (args, _, out, _, own) in zip(job.jobs, job.parts):
            mine, given = _split(given, len(args))
            results, outs = _split(outs, len(out))
            rooms, scratch = _split(scratch, len(own))
            self.codes.append(one.bind(mine, results, rooms))
        self.plan = sum((code.plan for code in self.codes), [])

    def load(self):
        for code in self.codes:
            code.load()

    def begin(self):
        for code in self.codes:
            code.begin()

    def slot(self, s):
        for code in self.codes:
            code.slot(s)

    def end(self):
        for code in self.codes:
            code.end()


class Join(Steps):
    plan, talks = [], None

    def __init__(self, parts, axis, number):
        self.parts, self.axis, self.number = parts, axis, number
        lengths = [w.shape[1 + axis] for w in parts]
        self.starts = [(sum(lengths[:i]), n) for i, n in enumerate(lengths)]
        self.shape = list(parts[0].shape[1:])
        self.shape[axis] = sum(lengths)

    def wants(self):
        n = len(self.parts)
        return list(self.parts), [ANY] * n, [ANY], [_sds(tuple(self.shape))], [pltpu.VMEM(tuple(self.shape), LOW), pltpu.SemaphoreType.DMA((n + 1,))]

    def bind(self, given, outs, scratch):
        code = Join(self.parts, self.axis, self.number)
        code.given, code.out, (code.own, code.sem) = given, outs[0], scratch
        return code

    def fetch(self, i):
        place = tuple(pl.ds(*self.starts[i]) if k == self.axis else ALL for k in range(2))
        return pltpu.make_async_copy(self.given[i].at[self.number], self.own.at[place], self.sem.at[i])

    def keep(self):
        return pltpu.make_async_copy(self.own, self.out, self.sem.at[len(self.given)])

    def load(self):
        for i in range(len(self.given)):
            self.fetch(i).start()

    def begin(self):
        for i in range(len(self.given)):
            self.fetch(i).wait()
        self.keep().start()

    def end(self):
        self.keep().wait()


class Exchange:
    def __init__(self, pairs, kinds, plan, talks, side):
        assert side == 4
        self.pairs, self.kinds, self.plan, self.talks, self.side = pairs, kinds, plan, talks, side
        self.work = [(k, c) for k in range(len(kinds)) for c in range(kinds[k].chunks)]

    def wants(self):
        scratch, side = [], self.side
        for kind in self.kinds:
            sizes = [kind.shape] * 2 + [kind.buffer(places, halves) for places in (side, 1) for halves in (1, 1, 2, 2)] + [kind.shape] * (not self.pairs)
            scratch += [pltpu.VMEM((kind.chunks, *size), LOW) for size in sizes]
        n, args = len(self.work), [a for pair in self.pairs for a in pair]
        scratch += [pltpu.SemaphoreType.DMA((n,))] + [pltpu.SemaphoreType.DMA((n, 9))] * 2
        results = [k.result for k in self.kinds]
        return args, [ANY] * len(args), [_spec(r) for r in results], [_sds(r) for r in results], scratch

    def bind(self, given, outs, scratch):
        return Exchanging(self, given, outs, scratch)


class Exchanging(Steps):
    def __init__(self, job, given, outs, scratch):
        self.job, self.given, self.outs, self.plan, self.side = job, given, outs, job.plan, job.side
        *buffers, self.load_sem, self.send_sem, self.recv_sem = scratch
        per = len(buffers) // len(job.kinds)
        self.buffers = [buffers[k * per : k * per + per] for k in range(len(job.kinds))]

    def load(self):
        if self.given:
            for n in range(len(self.job.work)):
                self.fetch(n).start()

    def begin(self):
        if self.given:
            for n in range(len(self.job.work)):
                self.copy(n, 0).start()

    def end(self):
        for n in range(len(self.job.work)):
            for event in range(9):
                self.copy(n, event).wait_send()

    def inside(self, c):
        return self.buffers[0][0].at[c], self.buffers[0][-1].at[c]

    def filled(self, c):
        self.copy(c, 0).start()

    def fetch(self, n):
        k, c = self.job.work[n]
        return pltpu.make_async_copy(self.given[2 * k].at[self.job.kinds[k].part(c)], self.buffers[k][0].at[c], self.load_sem.at[n])

    def copy(self, n, event):
        k, c = self.job.work[n] if self.given else (0, n)
        kind, side = self.job.kinds[k], self.side
        near = _near(side)
        if event == 0:
            src, to = self.given[2 * k + 1].at[kind.part(c)] if self.given else self.inside(c)[1], near[0]
        else:
            axis, what = divmod(event - 1, 4)
            places = 1 if axis else side
            part = [kind.at(2 * places, places, 0), kind.at(2 * places, places, 1), kind.at(places, places), kind.at(3 * places, places)][what]
            src, to = self.buffers[k][0].at[c].at[part], near[1 + 2 * axis + what % 2]
        return pltpu.make_async_remote_copy(src_ref=src, dst_ref=self.buffers[k][event + 1].at[c], send_sem=self.send_sem.at[n, event],
                                            recv_sem=self.recv_sem.at[n, event], device_id={"dp": to}, device_id_type=MESH)

    def stage(self, n, stage):
        k, c = self.job.work[n]
        kind, side = self.job.kinds[k], self.side
        own, far, up1, down1, next1, last1, up2, down2, next2, last2, *_ = (b.at[c] for b in self.buffers[k])

        def total(index, others):
            out = own[index].astype(WIDE) + far[index].astype(WIDE)
            for ref, at in others:
                out += ref[at].astype(WIDE)
            return out

        def ring(axis, place, inner, at):
            first, d2s = 1 + 4 * axis, 1 if axis else side
            up, down = (up2, down2) if axis else (up1, down1)

            def put(which, half, others):
                def one(i):
                    index = kind.at(place(which, i), 1, half)
                    own[index] = _low(total(index, inner(which, half) + [(ref, at(i)) for ref in others]))

                if axis:
                    one(0)
                else:
                    _loop(0, d2s, one)

            if stage == 2 * axis:
                put(2, None, [])
                self.copy(n, first).start()
                self.copy(n, first + 1).start()
            else:
                self.copy(n, first).wait_recv()
                put(1, 0, [up])
                put(1, 1, [])
                self.copy(n, first + 2).start()
                self.copy(n, first + 1).wait_recv()
                put(3, 0, [])
                put(3, 1, [down])
                self.copy(n, first + 3).start()

        both = lambda d2, half: [(ref, kind.at(d2, 1, half)) for ref in (next1, last1)]
        if stage == 0:
            if self.given:
                self.fetch(n).wait()
            self.copy(n, 0).wait_recv()
        if stage == 2:
            for event in (3, 4):
                self.copy(n, event).wait_recv()
        if stage < 2:
            ring(0, lambda which, i: which * side + i, lambda which, half: [], lambda i: kind.at(i, 1))
        elif stage < 4:
            ring(1, lambda which, i: which, both, lambda i: kind.at())
        else:
            for event in (7, 8):
                self.copy(n, event).wait_recv()
            self.outs[k][kind.part(c)] = _low(total(kind.at(0, 1), both(0, None) + [(next2, kind.at()), (last2, kind.at())]))


class Gather:
    def __init__(self, parts, axis, cut, number, plan, talks, side):
        self.join, self.cut, self.plan, self.talks, self.side = Join(parts, axis, number), cut, plan, talks, side
        self.shard = self.join.shape
        self.chunk = self.shard[cut] // len(plan)
        self.table, sides = [], range(side)

        def event(d1, d2, to, half=None):
            self.table.append((d1, d2, to, half))
            return len(self.table) - 1

        core, up1, down1, up2, down2 = range(5)
        last = side - 1
        self.second = [event(0, 0, up2), event(0, 0, down2)]
        self.second_on = [event(0, last, up2, 0), event(0, 1, down2, 1)]
        self.up, self.down = ([event(0, i, to) for i in sides] for to in (up1, down1))
        self.on = [event(last, i, up1) if i < 2 else event(1, i, down1) for i in sides]
        self.core = [[event(i, k, core) for k in sides] for i in sides]

    def wants(self):
        args, ins, out, _, scratch = self.join.wants()
        sems = [pltpu.SemaphoreType.DMA((len(self.plan), len(self.table)))] * 2
        return args, ins, out, [_sds((self.side, self.side, 2, *self.shard))], scratch + sems

    def bind(self, given, outs, scratch):
        return Gathering(self, given, outs, scratch)


class Gathering(Steps):
    def __init__(self, job, given, outs, scratch):
        self.job, self.out, self.plan, self.side = job, outs[0], job.plan, job.side
        *room, self.send_sem, self.recv_sem = scratch
        self.mine = job.join.bind(given, [self.shard(0, 0)], room)
        self.load, self.begin = self.mine.load, self.mine.begin

    def shard(self, d1, d2):
        x, y, c = _place()
        move = jnp.where(c == 0, d2, d1)
        return self.out.at[lax.rem(x + move, self.side), lax.rem(y + d1 + d2 - move, self.side), c]

    def copy(self, n, event):
        job = self.job
        d1, d2, to, half = job.table[event]
        part = (n * job.chunk, job.chunk) if half is None else (n * job.chunk + half * (job.chunk // 2), job.chunk // 2)
        part = tuple(pl.ds(*part) if k == job.cut else ALL for k in range(2))
        dst = self.shard(d1, d2).at[part]
        src = self.mine.own.at[part] if d1 == d2 == 0 else dst
        return pltpu.make_async_remote_copy(src_ref=src, dst_ref=dst, send_sem=self.send_sem.at[n, event], recv_sem=self.recv_sem.at[n, event],
                                            device_id={"dp": _near(self.side)[to]}, device_id_type=MESH)

    def load(self):
        for i in range(len(self.given)):
            self.fetch(i).start()

    def end(self):
        for n in range(len(self.plan)):
            for event in range(len(self.job.table)):
                self.copy(n, event).wait_send()
        self.mine.end()

    def stage(self, n, stage):
        job, side = self.job, self.side
        order = (0, side - 1, 1, 2)

        def start(*events):
            for event in events:
                self.copy(n, event).start()

        def came(event):
            self.copy(n, event).wait_recv()

        def forward(i):
            start(job.up[i], job.down[i], job.core[0][i])

        if stage == 0:
            start(*job.second)
            forward(0)
        elif stage == 1:
            for event, on, i in zip(job.second, job.second_on, order[1:]):
                came(event)
                start(on)
                forward(i)
        elif stage == 2:
            for event in job.second_on:
                came(event)
            forward(2)
        elif stage == 3:
            for i in order:
                for k, (event, d1) in enumerate(((job.up[i], side - 1), (job.down[i], 1))):
                    came(event)
                    start(*([job.on[i]] if (i < 2) == (k == 0) else []), job.core[d1][i])
        elif stage == 4:
            for i in order:
                came(job.on[i])
                start(job.core[2][i])
        else:
            for events in job.core:
                for event in events:
                    came(event)


def alone(job, name):
    other = Beside(job)

    def kernel(*refs):
        _, code = other.split(refs, 0, 0)
        code.before(0, 0)
        code.after(0, 0)

    return _call(kernel, name, (), other.ins, other.outs, other.shapes, other.scratch, COST, other.args, talks=other.talks)


def clip(grads, count, devices, talks):
    block = (8, HEAD)

    def kernel(*refs):
        gs, (out_ref, mine, slots, send_sem, recv_sem) = refs[: len(grads)], refs[len(grads) :]
        me = lax.axis_index("dp")
        barrier = pltpu.get_barrier_semaphore()
        to = lambda k: {"dp": lax.rem(me + k, devices)}
        each = functools.partial(_loop, 1, devices)
        each(lambda k: pl.semaphore_signal(barrier, inc=1, device_id=to(k), device_id_type=MESH))
        mine[:] = jnp.broadcast_to(sum(jnp.sum(g[:].astype(WIDE) ** 2) for g in gs), block)
        pl.semaphore_wait(barrier, devices - 1)

        def copy(k, slot):
            return pltpu.make_async_remote_copy(src_ref=mine, dst_ref=slots.at[slot], send_sem=send_sem.at[k], recv_sem=recv_sem.at[slot],
                                                device_id=to(k), device_id_type=MESH)

        each(lambda k: copy(k, me).start())
        slots[pl.ds(me, 1)] = mine[:][None]
        each(lambda k: copy(k, lax.rem(me + devices - k, devices)).wait_recv())
        each(lambda k: copy(k, me).wait_send())
        out_ref[:] = jnp.minimum(1.0, 0.5 * lax.rsqrt(jnp.sum(slots[:], axis=0) / count + 1e-30))

    return _call(kernel, "clip", (), [ONCHIP] * len(grads), [ONCHIP], [_sds(block, WIDE)],
                 [pltpu.VMEM(block, WIDE), pltpu.VMEM((devices, *block), WIDE)] + [pltpu.SemaphoreType.DMA((devices,))] * 2, COST, grads, talks=talks)[0]


def adamw(factor, weights, ms, vs, grads, chips):
    steps, layers, count = 4, len(grads), len(weights)
    blocks, maps = [], []
    for w in weights:
        l, r, n = w.shape
        tall = r % (steps * 16) == 0
        blocks.append((l, r // steps, n) if tall else (l, r, n // steps))
        maps.append("a1" if tall else "a2")
    specs = [_spec(b, **{m: _first}) for b, m in zip(blocks, maps)]
    rd, ro = blocks[6][1], blocks[3][1]
    g_specs, g_args = [], []
    for qkv, rows, gu in grads:
        d = rows.shape[1]
        after = functools.partial(lambda off, i: off + i, steps * rd // ro)
        g_specs += [_spec((*qkv.shape[:2], qkv.shape[2] // steps), a2=_first), _spec((rd, d), a0=_first), _spec((ro, d), a0=after), _spec((gu.shape[0], gu.shape[1] // steps), a1=_first)]
        g_args += [qkv, rows, rows, gu]

    def kernel(factor_ref, *refs):
        ws, m_refs, v_refs, gs, outs = _split(refs, *[count] * 3, len(g_args))
        factor = factor_ref[:1, :1]
        for l in range(layers):
            (qkv, down, out, gu), gs = gs[:4], gs[4:]
            per = chips // steps
            wide = gu.shape[1] // (2 * per)
            halves = [jnp.concatenate([gu[:, pl.ds((2 * p + k) * wide, wide)] for p in range(per)], axis=1) for k in range(2)]
            for i, g in enumerate((*[qkv[k] for k in range(3)], out[:], *halves, down[:])):
                g = g.astype(WIDE) * factor
                m = 0.9 * m_refs[i][l] + 0.1 * g
                v = 0.95 * v_refs[i][l] + 0.05 * g * g
                w = ws[i][l].astype(WIDE)
                outs[i][l] = _low(w - 0.02 * (m * lax.rsqrt(v + 1e-8) + 0.1 * w))
                outs[count + i][l] = m
                outs[2 * count + i][l] = v

    shapes = [_sds(w.shape, kind) for kind in (LOW, WIDE, WIDE) for w in weights]
    return _call(kernel, "adamw", (steps,), [_spec(factor.shape)] + specs * 3 + g_specs, specs * 3, shapes, [], COST, [factor, *weights, *ms, *vs, *g_args])


def solution(mesh):
    devices = mesh.shape["dp"]
    side = math.isqrt(devices // 2)
    chips = side * side

    def step(x, dy, *arrays):
        weights, ms, vs, _ = _split(arrays, *[len(arrays) // 3] * 3)
        wq, wk, wv, wo, wg, wu, wd = weights
        layers = wq.shape[0]
        x, dy = x[0], dy[0]
        t, d = x.shape
        f, ff = wq.shape[2], wg.shape[2]
        heads = f // HEAD
        rd, ro = wd.shape[1], wo.shape[1]
        *_, c = _place()
        chip = _chip(jnp.arange(chips, dtype=jnp.int32), side)
        other = chip.reshape(side, side).T.reshape(-1)
        per = d // devices
        rel = jnp.concatenate([chip * 2 + c, other * 2 + 1 - c])
        rel = (rel[:, None] * per + jnp.arange(per, dtype=jnp.int32)).reshape(-1)
        onehot = _low(jnp.arange(d, dtype=jnp.int32)[:, None] == rel)
        relative = lambda a: _low(_dot(onehot, a, 0, 1))
        half = HEAD // 2
        angle = jnp.arange(t, dtype=WIDE)[:, None] * THETA ** (-jnp.arange(half, dtype=WIDE) / half)
        cos = jnp.concatenate([jnp.cos(angle)] * 2, 1)
        sin = jnp.concatenate([-jnp.sin(angle), jnp.sin(angle)], 1)
        gather = lambda shard, tiled=True: lax.all_gather(shard, "dp", axis=0, tiled=tiled)
        qkv_job = lambda n, *plan: Gather((wq, wk, wv), 1, 1, n, _plan(*plan), 6 + n, side)
        w, gu_shard, rows_shard = alone(Jobs(qkv_job(0, "123456", "234567"), Join((wg, wu), 1, 1), Join((wd, wo), 0, 1)), "gathered")
        w_qkv = [w.reshape(d, -1)]
        w_gu = [gather(jnp.concatenate([wg[0], wu[0]], 1)), gather(gu_shard)]
        rows = [None, gather(rows_shard, False)]
        h, kept, job = x, [], Gather((wd, wo), 0, 0, 0, _plan("023578", "034789"), 1, side)
        for n in range(layers):
            qkv = qkv_forward(h, w_qkv[n], cos, sin)
            out, out_t, lse, *more = attend(qkv, heads, job)
            if job:
                rows[n], job = more[0].reshape(devices, -1, d), None
            h2, b, b_t = out_forward(h, out, rows[n], ro)
            kept.append((h, qkv, out_t, lse, h2, b, b_t))
            if n < layers - 1:
                h, more = mlp_forward(h2, b, w_gu[n], rows[n], rd, qkv_job(1, "012345", "123456"))
                w_qkv.append(more.reshape(d, -1))
        g_gu, g_rows, g_qkv = ([None] * layers for _ in range(3))
        scatter = lambda a: lax.psum_scatter(a, "dp", scatter_dimension=0, tiled=True)
        dh = dy
        for n in reversed(range(layers)):
            h, qkv, out_t, lse, h2, b, b_t = kept[n]
            last, job = n == 0, None
            rows_kind = lambda: Kind(pair[0].shape, 0, 1, 1, 2, side)
            if last:
                job = Exchange([pair, two], [rows_kind(), Kind(two[0].shape, 1, 2, 2, 2, side)], _plan("3579b", "468ac", "68ace", "79bdf"), 3, side)
            dh2, gu, *pair = mlp_back(h2, b, b_t, dh, w_gu[n], rows[n], rd, side, job)
            if last:
                pair, (g_rows[1], g_qkv[1]), _ = _split(pair, 2, 2)
            dot, delta, *pair = out_back(dh2, out_t, rows[n], ro, pair, heads, side)
            if last:
                dot, g_gu[1] = lax.optimization_barrier((dot, g_gu[1]))
                job = Exchange([pair], [rows_kind()], _plan("358cf", "57bfh"), 2, side)
            g_gu[n] = scatter(gu)
            dq, dk, dv, *more = attend_back(qkv, dot, lse, delta, cos, sin, heads, job)
            a_rel = relative(_normed(h))
            if last:
                g_rows[n] = more[0]
                g_qkv[n] = qkv_back(h, a_rel, dh2, (dq, dk, dv), w_qkv[n], (_plan("12345", "23456", "34567", "45678"), 4), side)[0]
            else:
                *two, dh = qkv_back(h, a_rel, dh2, (dq, dk, dv), w_qkv[n], None, side)
        grads = [(g_qkv[n], g_rows[n][0], g_gu[n]) for n in range(layers)]
        factor = clip([g for one in grads for g in one], sum(w.size for w in weights) * devices, devices, 8)
        return tuple(adamw(factor, weights, ms, vs, grads, chips))

    states, cut = P(("rep", "dp"), None, None), P(None, "dp", None)
    return jax.shard_map(step, mesh=mesh, in_specs=(states, states) + (cut,) * 21, out_specs=(P("rep", "dp", None),) * 21, check_vma=False)
```

```python
import functools
import math

import jax
import jax.numpy as jnp
from jax import lax
from jax.experimental import pallas as pl
from jax.experimental.pallas import tpu as pltpu
from jax.sharding import PartitionSpec as P

HEAD, THETA = 128, 10000
NEG = -1e30
HIDDEN = 2 * NEG
LOG2E = 1.4426950408889634
VMEM = 62 * 2**20
SHEET = 16
TILE, WIDTH = 256, 512
LOW, WIDE = jnp.bfloat16, jnp.float32
ALL = slice(None)
COST = 10**9
ANY = pl.BlockSpec(memory_space=pl.ANY)
ONCHIP = pl.BlockSpec(memory_space=pltpu.VMEM)
MESH = pl.DeviceIdType.MESH


def _dot(a, b, ca, cb):
    return lax.dot_general(a, b, (((ca,), (cb,)), ((), ())), preferred_element_type=WIDE)


def _nn(a, b):
    return _dot(a, b, 1, 0)


def _nt(a, b):
    return _dot(a, b, 1, 1)


def _tn(a, b):
    return _dot(a, b, 0, 0)


def _low(a):
    return a.astype(LOW)


def _sds(shape, dtype=LOW):
    return jax.ShapeDtypeStruct(shape, dtype)


def _spec(shape, **index):
    return pl.BlockSpec(shape, lambda *g: tuple(index[f"a{k}"](*g) if f"a{k}" in index else 0 for k in range(len(shape))))


def _first(i, *_):
    return i


def _loop(a, b, body):
    lax.fori_loop(a, b, lambda i, _: body(i), None)


def _split(refs, *counts):
    groups = []
    for n in counts:
        groups.append(refs[:n])
        refs = refs[n:]
    return (*groups, refs)


def _call(kernel, name, grid, ins, outs, shapes, scratch, flops, args, aliases=None, talks=None):
    nbytes = sum(math.prod(a.shape) * a.dtype.itemsize for a in (*args, *shapes))
    params = dict(vmem_limit_bytes=VMEM, dimension_semantics=("arbitrary",) * len(grid))
    if talks is not None:
        params.update(collective_id=talks, has_side_effects=True)
    return pl.pallas_call(
        kernel,
        grid_spec=pl.GridSpec(grid=grid, in_specs=ins, out_specs=outs, scratch_shapes=scratch),
        out_shape=shapes,
        compiler_params=pltpu.CompilerParams(**params),
        cost_estimate=pl.CostEstimate(flops=flops, transcendentals=0, bytes_accessed=nbytes),
        input_output_aliases=aliases or {},
        name=name,
    )(*args)


def _clear(acc, i):
    @pl.when(i == 0)
    def _():
        acc[:] = jnp.zeros_like(acc)


def _scale(wide):
    return lax.rsqrt(jnp.mean(wide**2, -1, keepdims=True) + 1e-6)


def _normed(h):
    wide = h.astype(WIDE)
    return _low(wide * _scale(wide))


def _norm_back(h, d):
    wide, d = h.astype(WIDE), d.astype(WIDE)
    scale = _scale(wide)
    inner = jnp.mean(d * wide, -1, keepdims=True)
    return _low(d * scale - wide * (scale * scale * scale * inner))


def _swap(one):
    return pltpu.roll(one, HEAD // 2, 1)


def _rows(ref, d):
    n, m = ref.shape[0] // SHEET, ref.shape[1] // d
    return jnp.concatenate([ref[k * SHEET : k * SHEET + SHEET, j * d : j * d + d] for k in range(n) for j in range(m)], axis=0)


def _heads(n):
    return [slice(i * HEAD, i * HEAD + HEAD) for i in range(n)]


def qkv_forward(h, w, cos, sin):
    t, d = h.shape
    width = w.shape[1]
    wide = 2 * WIDTH
    n = width // wide

    def kernel(h_ref, w_ref, cos_ref, sin_ref, o_ref, a_s):
        i = pl.program_id(0)

        @pl.when(i == 0)
        def _():
            a_s[:] = _normed(h_ref[:])

        def run(turn):
            for k in range(0, wide, TILE):
                y = _low(_nn(a_s[:], w_ref[:, k : k + TILE]))
                if turn:
                    y = y.astype(WIDE)
                    y = _low(jnp.concatenate([y[:, c] * cos_ref[:] + _swap(y[:, c]) * sin_ref[:] for c in _heads(TILE // HEAD)], axis=1))
                o_ref[:, k : k + TILE] = y

        pl.when(i < n - n // 3)(lambda: run(True))
        pl.when(i >= n - n // 3)(lambda: run(False))

    angle = _spec((t, HEAD))
    return _call(kernel, "qkv", (n,), [_spec((t, d)), _spec((d, wide), a1=_first), angle, angle], [_spec((t, wide), a1=_first)],
                 [_sds((t, width))], [pltpu.VMEM((t, d), LOW)], 2 * t * d * width, [h, w, cos, sin])[0]


def attend(qkv, heads, beside=None):
    t, f = qkv.shape[0], heads * HEAD
    bq = bk = TILE
    group = extra = 8
    scale = HEAD**-0.5
    e = scale * LOG2E

    other, n = Beside(beside), t // bq

    def kernel(q_ref, k_ref, v_ref, *rest):
        (o_ref, ot_ref, lse_ref, top_s, mix_s), job = other.split(rest, 0, 3)
        iq = pl.program_id(0)
        job.before(2 * iq, 2 * n - 1, False)
        top_s[:] = jnp.full(top_s.shape, NEG, WIDE)
        mix_s[:] = jnp.zeros(mix_s.shape, WIDE)
        ones = jnp.ones((extra, bk), LOW)
        cols = _heads(heads)

        def block(j, masked):
            here = pl.ds(pl.multiple_of(j * bk, bk), bk)
            scores = [_nt(k_ref[here, c], q_ref[:, c]) for c in cols]
            weights, keeps = [], []
            for i, s in enumerate(scores):
                if masked:
                    ok = lax.broadcasted_iota(jnp.int32, (bk, bq), 1) >= lax.broadcasted_iota(jnp.int32, (bk, bq), 0)
                    s = jnp.where(ok, s, HIDDEN)
                old = top_s[i : i + 1, :]
                top = jnp.maximum(old, s.max(axis=0, keepdims=True))
                top_s[pl.ds(i, 1), :] = top
                weights.append(_low(jnp.exp2((s - top) * e)))
                keeps.append(jnp.exp2((old - top) * e))
            for i, (p, keep) in enumerate(zip(weights, keeps)):
                values = jnp.concatenate([v_ref[here, cols[i]].T, ones], axis=0)
                mix_s[i] = mix_s[i] * keep + _nn(values, p)

        _loop(0, iq, lambda j: block(j, False))
        job.before(2 * iq + 1, 2 * n - 1, True)
        block(iq, True)
        for i, c in enumerate(cols):
            total = mix_s[i, HEAD : HEAD + 1, :]
            out = _low(mix_s[i, :HEAD, :] * (1 / total))
            ot_ref[c, :] = out
            o_ref[:, c] = out.T
            lse_ref[i // group, i % group : i % group + 1, :] = top_s[i : i + 1, :] * scale + jnp.log(total)
        job.after(2 * iq + 1, 2 * n - 1)

    keys = [_spec((t, f), a1=functools.partial(lambda g, i: g, g)) for g in (1, 2)]
    return _call(kernel, "attend", (n,), [_spec((bq, f), a0=_first), *keys, *other.ins],
                 [_spec((bq, f), a0=_first), _spec((f, bq), a1=_first), _spec((heads // group, group, bq), a2=_first), *other.outs],
                 [_sds((t, f)), _sds((f, t)), _sds((heads // group, group, t), WIDE), *other.shapes],
                 [pltpu.VMEM((heads, bq), WIDE), pltpu.VMEM((heads, HEAD + extra, bq), WIDE), *other.scratch], 4 * t * t * f, [qkv] * 3 + other.args, talks=other.talks)


def attend_back(qkv, dot, lse, delta, cos, sin, heads, beside=None, a_rel=None):
    t, f = qkv.shape[0], heads * HEAD
    kb, bq, bk = lse.shape[1], TILE, TILE
    scale = HEAD**-0.5
    e = scale * LOG2E
    w = kb * HEAD
    nh, nq = heads // kb, t // bq
    other, inside = Beside(beside), int(a_rel is not None)

    def kernel(q_ref, k_ref, v_ref, dot_ref, lse_ref, delta_ref, cos_ref, sin_ref, *rest):
        refs, job = other.split(rest, inside, 3 - 3 * inside)
        iq, group = pl.program_id(1), pl.program_id(0)
        here = pl.ds(pl.multiple_of(iq * bq, bq), bq)
        if inside:
            a_ref, dq_s, dk_s, dv_s, all_s = refs
            dq_ref, dk_ref, dv_ref = all_s.at[0, here], all_s.at[1], all_s.at[2]
        else:
            dq_ref, dk_ref, dv_ref, dq_s, dk_s, dv_s = refs
        step, last = 2 * (group * nq + iq), 2 * nh * nq - 1
        job.before(step, last, False)
        cols = _heads(kb)

        @pl.when(iq == 0)
        def _():
            dk_s[:] = jnp.zeros_like(dk_s)
            dv_s[:] = jnp.zeros_like(dv_s)

        dq_s[:] = jnp.zeros_like(dq_s)
        lses = [lse_ref[0, i : i + 1, :] * LOG2E for i in range(kb)]
        deltas = [delta_ref[0, i : i + 1, :] for i in range(kb)]

        def block(j, masked):
            here = pl.ds(pl.multiple_of(j * bk, bk), bk)
            scores = [_nt(k_ref[here, c], q_ref[:, c]) for c in cols]
            dps = [_nn(v_ref[here, c], dot_ref[c, :]) for c in cols]
            for i, c in enumerate(cols):
                p = jnp.exp2(scores[i] * e - lses[i])
                if masked:
                    ok = lax.broadcasted_iota(jnp.int32, p.shape, 1) >= lax.broadcasted_iota(jnp.int32, p.shape, 0)
                    p = jnp.where(ok, p, 0.0)
                ds = _low(p * (dps[i] - deltas[i]))
                dv_s[here, c] += _nt(_low(p), dot_ref[c, :])
                dk_s[here, c] += _nn(ds, q_ref[:, c])
                dq_s[i] += _nn(k_ref[here, c].T, ds)

        _loop(0, iq, lambda j: block(j, False))
        job.before(step + 1, last, True)
        block(iq, True)

        def back(g, at):
            g = _low(g * scale).astype(WIDE)
            return _low(g * cos_ref[at, :] - _swap(g) * sin_ref[at, :])

        for i, c in enumerate(cols):
            dq_ref[:, c] = back(dq_s[i].T, here)

        @pl.when(iq == nq - 1)
        def _():
            for c in cols:
                dk_ref[:, c] = back(dk_s[:, c], ALL)
            dv_ref[:] = _low(dv_s[:])
            if inside:
                exchange = job.codes[-1]
                own, par = exchange.inside(group)
                for g in range(3):
                    res = _low(_nn(a_ref[:], all_s[g]))
                    own[g] = res[: own.shape[1]]
                    par[g] = res[own.shape[1] :]
                exchange.filled(group)

        job.after(step + 1, last)

    head = lambda h, i: h
    query = lambda h, i: i
    stats = _spec((1, kb, bq), a0=head, a2=query)
    keys = [_spec((t, w), a1=functools.partial(lambda g, h, i: g * nh + h, g)) for g in range(3)]
    ins = [_spec((bq, w), a0=query, a1=head), *keys[1:], _spec((w, bq), a0=head, a1=query), stats, stats] + [_spec((t, HEAD))] * 2
    args, sums = [qkv, qkv, qkv, dot, lse, delta, cos, sin], [pltpu.VMEM((kb, HEAD, bq), WIDE), pltpu.VMEM((t, w), WIDE), pltpu.VMEM((t, w), WIDE)]
    if inside:
        ins, args, outs, shapes, sums = [*ins, _spec(a_rel.shape)], [*args, a_rel], [], [], [*sums, pltpu.VMEM((3, t, w), LOW)]
    else:
        outs, shapes = [ins[0], keys[0], keys[0]], [_sds((t, f))] * 3
    return _call(kernel, "attend_back", (nh, nq), ins + other.ins, outs + other.outs, shapes + other.shapes, sums + other.scratch,
                 10 * t * t * f, args + other.args, talks=other.talks)


def out_forward(h, out, rows, r):
    t, d = h.shape
    f = out.shape[1]
    tiles, first = rows
    wide = r // SHEET * d

    def kernel(h_ref, out_ref, w_ref, h_out, b_out, bt_out):
        h = h_ref[:] + _low(_nn(out_ref[:], _rows(w_ref, d)))
        h_out[:] = h
        b = _normed(h)
        b_out[:] = b
        bt_out[:] = b.T

    row = _spec((WIDTH, d), a0=_first)
    return _call(kernel, "out", (t // WIDTH,), [row, _spec((WIDTH, f), a0=_first), _spec((tiles.shape[0], wide), a1=lambda i: first // wide)],
                 [row, row, _spec((d, WIDTH), a1=_first)], [_sds((t, d))] * 2 + [_sds((d, t))], [], 2 * t * d * f, [h, out, tiles])


def out_back(dh, out_t, rows, r, grads, heads, side):
    t, d = dh.shape
    f = heads * HEAD
    wide, chips = 2 * WIDTH, side * side
    n, group, m = f // wide, wide // HEAD, len(grads)
    at = grads[0].shape[1] // r - 1
    tiles, first = rows
    across = r // SHEET * d

    def kernel(dh_ref, ot_ref, w_ref, *rest):
        _, (dot_ref, delta_ref), outs, (res_s,) = _split(rest, m, 2, m)
        i = pl.program_id(0)
        d_out = _low(_nt(_rows(w_ref, d), dh_ref[:]))
        dot_ref[:] = d_out
        prod = d_out.astype(WIDE) * ot_ref[:].astype(WIDE)
        for k, c in enumerate(_heads(group)):
            delta_ref[0, k : k + 1, :] = jnp.sum(prod[c, :], axis=0, keepdims=True)
        res_s[pl.ds(pl.multiple_of(i * wide, wide), wide), :] = _low(_nn(ot_ref[:], dh_ref[:]))

        @pl.when(i == n - 1)
        def _():
            *_, c = _place()
            rows_of = lambda j, c: res_s[pl.ds(pl.multiple_of((_chip(jnp.int32(j), side) * 2 + c) * r, r), r), :]
            for j in range(chips):
                outs[0][j] = rows_of(j, c)
                outs[1][(j % side) * side + j // side] = rows_of(j, 1 - c)

    block = _spec((wide, t), a0=_first)
    w_spec = _spec((wide // r * SHEET, across), a0=_first, a1=lambda i: first // across)
    return _call(kernel, "out_back", (n,), [_spec((t, d)), block, w_spec] + [ANY] * m,
                 [block, _spec((1, group, t), a0=_first)] + [_spec((chips, r, d), a1=lambda *_: at)] * m,
                 [_sds((f, t)), _sds((n, group, t), WIDE)] + [_sds(g.shape) for g in grads],
                 [pltpu.VMEM((f, d), LOW)], 4 * t * d * f, [dh, out_t, tiles, *grads], aliases={3 + k: 2 + k for k in range(m)})


def mlp_forward(h, b, gu, rows, r, ff, beside=None):
    t, d = h.shape
    wide = 2 * WIDTH
    tiles, first = rows
    across = r // SHEET * d
    n = ff // wide
    other = Beside(beside)

    def kernel(h_ref, b_ref, g_ref, u_ref, d_ref, *rest):
        (o_ref, acc, act), job = other.split(rest, 0, 1)
        i = pl.program_id(0)
        job.before(i, n - 1)
        _clear(acc, i)
        for k in range(0, wide, TILE):
            gate, up = _nn(b_ref[:], g_ref[:, k : k + TILE]), _nn(b_ref[:], u_ref[:, k : k + TILE])
            act[:, k : k + TILE] = _low(gate * jax.nn.sigmoid(gate) * up)
        acc[:] += _nn(act[:], _rows(d_ref, d))

        @pl.when(i == n - 1)
        def _():
            o_ref[:] = h_ref[:] + _low(acc[:])

        job.after(i, n - 1)

    whole = _spec((t, d))
    return _call(kernel, "mlp", (n,), [whole, whole, _spec((d, wide), a1=_first), _spec((d, wide), a1=lambda i: n + i), _spec((wide // r * SHEET, across), a0=_first, a1=lambda i: first // across), *other.ins],
                 [whole, *other.outs], [_sds((t, d)), *other.shapes], [pltpu.VMEM((t, d), WIDE), pltpu.VMEM((t, wide), LOW), *other.scratch],
                 6 * t * d * ff, [h, b, gu, gu, tiles, *other.args], talks=other.talks)


def mlp_back(h, b, b_t, dy, gu, rows, r, deep, side, beside=None):
    t, d = h.shape
    wide, n = 2 * r, side * side
    tiles, first = rows
    across = r // SHEET * d
    other = Beside(beside)

    def kernel(h_ref, b_ref, bt_ref, dy_ref, g_ref, u_ref, d_ref, *rest):
        (dh_ref, gu_out, *d_out, acc, act, dgu, res), job = other.split(rest, 0, 4)
        i = pl.program_id(0)
        job.before(i, n - 1)
        _clear(acc, i)
        b, dy, down = b_ref[:], dy_ref[:], _rows(d_ref, d)
        for k in range(0, wide, TILE):
            gate, up = _nn(b, g_ref[:, k : k + TILE]), _nn(b, u_ref[:, k : k + TILE])
            dact = _low(_nt(dy, down[k : k + TILE, :])).astype(WIDE)
            sig = jax.nn.sigmoid(gate)
            silu = gate * sig
            act[:, k : k + TILE] = _low(silu * up)
            dgu[:, k : k + TILE] = _low(dact * up * (sig + silu * (1 - sig)))
            dgu[:, wide + k : wide + k + TILE] = _low(dact * silu)
        gu_out[:] = _low(_nn(bt_ref[:], dgu[:]))
        acc[:] += _nt(dgu[:, :wide], g_ref[:]) + _nt(dgu[:, wide:], u_ref[:])
        res[:] = _low(_tn(act[:], dy))
        *_, core = _place()
        for k, ref in enumerate(d_out):
            ref[0] = res[pl.ds(pl.multiple_of(jnp.where(core == k, 0, r), r), r), :]

        @pl.when(i == n - 1)
        def _():
            dh_ref[:] = dy_ref[:] + _norm_back(h_ref[:], _low(acc[:]))

        job.after(i, n - 1)

    row, col = _spec((t, d)), _spec((d, t))
    d_specs = [_spec((1, r, d), a0=functools.partial(lambda k, i: _back(i, side)[k], k)) for k in range(2)]
    return _call(kernel, "mlp_back", (n,),
                 [row, row, col, row, _spec((d, wide), a1=_first), _spec((d, wide), a1=lambda i: n + i), _spec((2 * SHEET, across), a0=_first, a1=lambda i: first // across)] + other.ins,
                 [row, _spec((d, 2 * wide), a1=_first)] + d_specs + other.outs, [_sds((t, d)), _sds((d, 2 * wide * n))] + [_sds((n, deep, d))] * 2 + other.shapes,
                 [pltpu.VMEM((t, d), WIDE), pltpu.VMEM((t, wide), LOW), pltpu.VMEM((t, 2 * wide), LOW), pltpu.VMEM((wide, d), LOW)] + other.scratch,
                 16 * t * d * wide * n, [h, b, b_t, dy, gu, gu, tiles, *other.args], talks=other.talks)


def qkv_back(h, a_rel, dh, dqkv, w):
    t, d = h.shape
    f, wide = dqkv[0].shape[1], WIDTH
    n, half, three = f // wide, d // 2, range(3)

    def kernel(h_ref, a_ref, dh_ref, *rest):
        i = pl.program_id(0)
        terms, ws, (own, par, out_ref, acc) = _split(rest, 3, 3)
        _clear(acc, i)
        for g in three:
            res = _low(_nn(a_ref[:], terms[g][:]))
            own[g] = res[:half]
            par[g] = res[half:]
        acc[:] += sum(_nt(terms[g][:], ws[g][:]) for g in three)

        @pl.when(i == n - 1)
        def _():
            out_ref[:] = dh_ref[:] + _norm_back(h_ref[:], _low(acc[:]))

    row, col = _spec((t, d)), _spec((t, wide), a1=_first)
    mats = [_spec((d, wide), a1=functools.partial(lambda g, i: g * n + i, g)) for g in three]
    return _call(kernel, "qkv_back", (n,), [row, _spec((d, t)), row, col, col, col, *mats], [_spec((3, half, wide), a2=_first)] * 2 + [row],
                 [_sds((3, half, f))] * 2 + [_sds((t, d))], [pltpu.VMEM((t, d), WIDE)], 12 * t * d * f, [h, a_rel, dh, *dqkv, *[w] * 3])


def _place():
    me, side = lax.axis_index("dp"), math.isqrt(lax.axis_size("dp") // 2)
    return lax.div(me, 2 * side), lax.rem(lax.div(me, 2), side), lax.rem(me, 2)


def _chip(place, side):
    x, y, c = _place()
    d1, d2 = lax.div(place, side), lax.rem(place, side)
    move = jnp.where(c == 0, d2, d1)
    return lax.rem(x + move, side) * side + lax.rem(y + d1 + d2 - move, side)


def _back(chip, side):
    x, y, c = _place()
    dx, dy = lax.rem(lax.div(chip, side) + side - x, side), lax.rem(lax.rem(chip, side) + side - y, side)
    along = jnp.where(c == 0, dy, dx)
    across = dx + dy - along
    return along * side + across, across * side + along


def _near(side):
    x, y, c = _place()
    place = lambda x, y, c: (x * side + y) * 2 + c
    near = [place(x, y, 1 - c)]
    for k in range(2):
        for by in (1, side - 1):
            move = jnp.where(c == k, 0, by)
            near.append(place(lax.rem(x + move, side), lax.rem(y + by - move, side), c))
    return near


def _greet(near):
    barrier = pltpu.get_barrier_semaphore()
    for to in near:
        pl.semaphore_signal(barrier, inc=1, device_id={"dp": to}, device_id_type=MESH)
    pl.semaphore_wait(barrier, len(near))


class Kind:
    def __init__(self, shape, places, split, chunk_axis, chunks, side):
        self.places, self.split, self.chunk_axis, self.chunks = places, split, chunk_axis, chunks
        self.chunk = shape[chunk_axis] // chunks
        self.shape = tuple(self.chunk if i == chunk_axis else n for i, n in enumerate(shape))
        self.per = shape[places] // (side * side)
        self.half = self.shape[split] // 2
        self.result = tuple(self.per if i == places else n for i, n in enumerate(shape))

    def buffer(self, places, halves):
        size = list(self.shape)
        size[self.places] = places * self.per
        size[self.split] = halves * self.half
        return tuple(size)

    def at(self, place=0, places=None, half=None):
        index = [ALL] * len(self.shape)
        if half is not None:
            index[self.split] = pl.ds(half * self.half, self.half)
        if places is not None:
            start = place * self.per
            index[self.places] = pl.ds(start if isinstance(start, int) else pl.multiple_of(start, self.per), places * self.per)
        return tuple(index)

    def part(self, c):
        index = [ALL] * len(self.shape)
        index[self.chunk_axis] = pl.ds(c * self.chunk, self.chunk)
        return tuple(index)


class Beside:
    def __init__(self, job):
        self.job, self.talks = job, job and job.talks
        self.args, self.ins, self.outs, self.shapes, self.scratch = job.wants() if job else ([], [], [], [], [])

    def split(self, refs, ins, outs):
        if not self.job:
            return refs, Nothing()
        mine, given, out, results, rest = _split(refs, ins, len(self.args), outs, len(self.outs))
        own, scratch = _split(rest, len(rest) - len(self.scratch))
        return (*mine, *out, *own), self.job.bind(given, results, scratch)


class Nothing:
    def before(self, step, last, amid=None):
        pass

    after = before


def _plan(*chunks):
    return [[int(digit, 36) for digit in steps] for steps in chunks]


class Steps:
    def before(self, step, last, amid=None):
        if not amid:

            @pl.when(step == 0)
            def _():
                self.load()
                _greet(_near(self.side))
                self.begin()

        for s in range(last + 1) if amid is None else range(int(amid), last + 1, 2):
            if any(s in steps for steps in self.plan):
                pl.when(step == s)(functools.partial(self.slot, s))

    def after(self, step, last):
        @pl.when(step == last)
        def _():
            for s in range(last + 1, 1 + max(max(steps) for steps in self.plan)):
                self.slot(s)
            self.end()

    def slot(self, s):
        here = [(stage, n) for n, steps in enumerate(self.plan) for stage, at in enumerate(steps) if at == s]
        for stage, n in sorted(here):
            self.stage(n, stage)


class Jobs:
    def __init__(self, *jobs):
        self.jobs, self.talks = jobs, jobs[0].talks

    def wants(self):
        self.parts = [job.wants() for job in self.jobs]
        return [sum((list(part[k]) for part in self.parts), []) for k in range(5)]

    def bind(self, given, outs, scratch):
        return Several(self, given, outs, scratch)


class Several(Steps):
    def __init__(self, job, given, outs, scratch):
        self.side, self.codes = job.jobs[0].side, []
        for one, (args, _, out, _, own) in zip(job.jobs, job.parts):
            mine, given = _split(given, len(args))
            results, outs = _split(outs, len(out))
            rooms, scratch = _split(scratch, len(own))
            self.codes.append(one.bind(mine, results, rooms))
        self.plan = sum((code.plan for code in self.codes), [])

    def load(self):
        for code in self.codes:
            code.load()

    def begin(self):
        for code in self.codes:
            code.begin()

    def slot(self, s):
        for code in self.codes:
            code.slot(s)

    def end(self):
        for code in self.codes:
            code.end()


class Join(Steps):
    plan, talks = [], None

    def __init__(self, parts, number):
        self.parts, self.number, self.pieces, at = parts, number, [], 0
        for i, w in enumerate(parts):
            _, tall, wide = w.shape
            for row in range(0, tall, SHEET):
                self.pieces.append((i, row, at, wide))
                at += wide
        self.shape = SHEET, at

    def wants(self):
        sems = pltpu.SemaphoreType.DMA((len(self.pieces) + 1,))
        return list(self.parts), [ANY] * len(self.parts), [ANY], [_sds(self.shape)], [pltpu.VMEM(self.shape, LOW), sems]

    def bind(self, given, outs, scratch):
        code = Join(self.parts, self.number)
        code.given, code.out, (code.own, code.sem) = given, outs[0], scratch
        return code

    def fetch(self, k):
        i, row, at, wide = self.pieces[k]
        return pltpu.make_async_copy(self.given[i].at[self.number, pl.ds(row, SHEET)], self.own.at[:, pl.ds(at, wide)], self.sem.at[k])

    def keep(self):
        return pltpu.make_async_copy(self.own, self.out, self.sem.at[len(self.pieces)])

    def load(self):
        for k in range(len(self.pieces)):
            self.fetch(k).start()

    def begin(self):
        for k in range(len(self.pieces)):
            self.fetch(k).wait()
        self.keep().start()

    def end(self):
        self.keep().wait()


class Exchange:
    def __init__(self, pairs, kinds, plan, talks, side):
        assert side == 4
        self.pairs, self.kinds, self.plan, self.talks, self.side = pairs, kinds, plan, talks, side
        self.work = [(k, c) for k in range(len(kinds)) for c in range(kinds[k].chunks)]

    def wants(self):
        scratch, side = [], self.side
        for kind in self.kinds:
            sizes = [kind.shape] * 2 + [kind.buffer(places, halves) for places in (side, 1) for halves in (1, 1, 2, 2)] + [kind.shape] * (not self.pairs)
            scratch += [pltpu.VMEM((kind.chunks, *size), LOW) for size in sizes]
        n, args = len(self.work), [a for pair in self.pairs for a in pair]
        scratch += [pltpu.SemaphoreType.DMA((n,))] + [pltpu.SemaphoreType.DMA((n, 9))] * 2
        results = [k.result for k in self.kinds]
        return args, [ANY] * len(args), [_spec(r) for r in results], [_sds(r) for r in results], scratch

    def bind(self, given, outs, scratch):
        return Exchanging(self, given, outs, scratch)


class Exchanging(Steps):
    def __init__(self, job, given, outs, scratch):
        self.job, self.given, self.outs, self.plan, self.side = job, given, outs, job.plan, job.side
        *buffers, self.load_sem, self.send_sem, self.recv_sem = scratch
        per = len(buffers) // len(job.kinds)
        self.buffers = [buffers[k * per : k * per + per] for k in range(len(job.kinds))]

    def load(self):
        if self.given:
            for n in range(len(self.job.work)):
                self.fetch(n).start()

    def begin(self):
        if self.given:
            for n in range(len(self.job.work)):
                self.copy(n, 0).start()

    def end(self):
        for n in range(len(self.job.work)):
            for event in range(9):
                self.copy(n, event).wait_send()

    def inside(self, c):
        return self.buffers[0][0].at[c], self.buffers[0][-1].at[c]

    def filled(self, c):
        self.copy(c, 0).start()

    def fetch(self, n):
        k, c = self.job.work[n]
        return pltpu.make_async_copy(self.given[2 * k].at[self.job.kinds[k].part(c)], self.buffers[k][0].at[c], self.load_sem.at[n])

    def copy(self, n, event):
        k, c = self.job.work[n] if self.given else (0, n)
        kind, side = self.job.kinds[k], self.side
        near = _near(side)
        if event == 0:
            src, to = self.given[2 * k + 1].at[kind.part(c)] if self.given else self.inside(c)[1], near[0]
        else:
            axis, what = divmod(event - 1, 4)
            places = 1 if axis else side
            part = [kind.at(2 * places, places, 0), kind.at(2 * places, places, 1), kind.at(places, places), kind.at(3 * places, places)][what]
            src, to = self.buffers[k][0].at[c].at[part], near[1 + 2 * axis + what % 2]
        return pltpu.make_async_remote_copy(src_ref=src, dst_ref=self.buffers[k][event + 1].at[c], send_sem=self.send_sem.at[n, event],
                                            recv_sem=self.recv_sem.at[n, event], device_id={"dp": to}, device_id_type=MESH)

    def stage(self, n, stage):
        k, c = self.job.work[n]
        kind, side = self.job.kinds[k], self.side
        own, far, up1, down1, next1, last1, up2, down2, next2, last2, *_ = (b.at[c] for b in self.buffers[k])

        def total(index, others):
            out = own[index].astype(WIDE) + far[index].astype(WIDE)
            for ref, at in others:
                out += ref[at].astype(WIDE)
            return out

        def ring(axis, place, inner, at):
            first, d2s = 1 + 4 * axis, 1 if axis else side
            up, down = (up2, down2) if axis else (up1, down1)

            def put(which, half, others):
                def one(i):
                    index = kind.at(place(which, i), 1, half)
                    own[index] = _low(total(index, inner(which, half) + [(ref, at(i)) for ref in others]))

                if axis:
                    one(0)
                else:
                    _loop(0, d2s, one)

            if stage == 2 * axis:
                put(2, None, [])
                self.copy(n, first).start()
                self.copy(n, first + 1).start()
            else:
                self.copy(n, first).wait_recv()
                put(1, 0, [up])
                put(1, 1, [])
                self.copy(n, first + 2).start()
                self.copy(n, first + 1).wait_recv()
                put(3, 0, [])
                put(3, 1, [down])
                self.copy(n, first + 3).start()

        both = lambda d2, half: [(ref, kind.at(d2, 1, half)) for ref in (next1, last1)]
        if stage == 0:
            if self.given:
                self.fetch(n).wait()
            self.copy(n, 0).wait_recv()
        if stage == 2:
            for event in (3, 4):
                self.copy(n, event).wait_recv()
        if stage < 2:
            ring(0, lambda which, i: which * side + i, lambda which, half: [], lambda i: kind.at(i, 1))
        elif stage < 4:
            ring(1, lambda which, i: which, both, lambda i: kind.at())
        else:
            for event in (7, 8):
                self.copy(n, event).wait_recv()
            self.outs[k][kind.part(c)] = _low(total(kind.at(0, 1), both(0, None) + [(next2, kind.at()), (last2, kind.at())]))


class Gather:
    def __init__(self, parts, number, plan, talks, side):
        self.join, self.plan, self.talks, self.side = Join(parts, number), plan, talks, side
        self.shard = self.join.shape
        self.chunk = self.shard[1] // len(plan)
        self.table, sides = [], range(side)

        def event(d1, d2, to, half=None):
            self.table.append((d1, d2, to, half))
            return len(self.table) - 1

        core, up1, down1, up2, down2 = range(5)
        last = side - 1
        self.second = [event(0, 0, up2), event(0, 0, down2)]
        self.second_on = [event(0, last, up2, 0), event(0, 1, down2, 1)]
        self.up, self.down = ([event(0, i, to) for i in sides] for to in (up1, down1))
        self.on = [event(last, i, up1) if i < 2 else event(1, i, down1) for i in sides]
        self.core = [[event(i, k, core) for k in sides] for i in sides]

    def wants(self):
        args, ins, out, _, scratch = self.join.wants()
        sems = [pltpu.SemaphoreType.DMA((len(self.plan), len(self.table)))] * 2
        return args, ins, out, [_sds((self.side, self.side, 2, *self.shard))], scratch + sems

    def bind(self, given, outs, scratch):
        return Gathering(self, given, outs, scratch)


class Gathering(Steps):
    def __init__(self, job, given, outs, scratch):
        self.job, self.out, self.plan, self.side = job, outs[0], job.plan, job.side
        *room, self.send_sem, self.recv_sem = scratch
        self.mine = job.join.bind(given, [self.shard(0, 0)], room)
        self.load, self.begin = self.mine.load, self.mine.begin

    def shard(self, d1, d2):
        x, y, c = _place()
        move = jnp.where(c == 0, d2, d1)
        return self.out.at[lax.rem(x + move, self.side), lax.rem(y + d1 + d2 - move, self.side), c]

    def copy(self, n, event):
        job = self.job
        d1, d2, to, half = job.table[event]
        part = (n * job.chunk, job.chunk) if half is None else (n * job.chunk + half * (job.chunk // 2), job.chunk // 2)
        part = ALL, pl.ds(*part)
        dst = self.shard(d1, d2).at[part]
        src = self.mine.own.at[part] if d1 == d2 == 0 else dst
        return pltpu.make_async_remote_copy(src_ref=src, dst_ref=dst, send_sem=self.send_sem.at[n, event], recv_sem=self.recv_sem.at[n, event],
                                            device_id={"dp": _near(self.side)[to]}, device_id_type=MESH)

    def load(self):
        for i in range(len(self.given)):
            self.fetch(i).start()

    def end(self):
        for n in range(len(self.plan)):
            for event in range(len(self.job.table)):
                self.copy(n, event).wait_send()
        self.mine.end()

    def stage(self, n, stage):
        job, side = self.job, self.side
        order = (0, side - 1, 1, 2)

        def start(*events):
            for event in events:
                self.copy(n, event).start()

        def came(event):
            self.copy(n, event).wait_recv()

        def forward(i):
            start(job.up[i], job.down[i], job.core[0][i])

        if stage == 0:
            start(*job.second)
            forward(0)
        elif stage == 1:
            for event, on, i in zip(job.second, job.second_on, order[1:]):
                came(event)
                start(on)
                forward(i)
        elif stage == 2:
            for event in job.second_on:
                came(event)
            forward(2)
        elif stage == 3:
            for i in order:
                for k, (event, d1) in enumerate(((job.up[i], side - 1), (job.down[i], 1))):
                    came(event)
                    start(*([job.on[i]] if (i < 2) == (k == 0) else []), job.core[d1][i])
        elif stage == 4:
            for i in order:
                came(job.on[i])
                start(job.core[2][i])
        else:
            for events in job.core:
                for event in events:
                    came(event)


def alone(job, name):
    other = Beside(job)

    def kernel(*refs):
        _, code = other.split(refs, 0, 0)
        if job.talks is None:
            code.load()
            code.begin()
            code.end()
        else:
            code.before(0, 0)
            code.after(0, 0)

    return _call(kernel, name, (), other.ins, other.outs, other.shapes, other.scratch, COST, other.args, talks=other.talks)


def clip(grads, count, devices, talks):
    block = (8, HEAD)

    def kernel(*refs):
        gs, (out_ref, mine, slots, send_sem, recv_sem) = refs[: len(grads)], refs[len(grads) :]
        me = lax.axis_index("dp")
        barrier = pltpu.get_barrier_semaphore()
        to = lambda k: {"dp": lax.rem(me + k, devices)}
        each = functools.partial(_loop, 1, devices)
        each(lambda k: pl.semaphore_signal(barrier, inc=1, device_id=to(k), device_id_type=MESH))
        mine[:] = jnp.broadcast_to(sum(jnp.sum(g[:].astype(WIDE) ** 2) for g in gs), block)
        pl.semaphore_wait(barrier, devices - 1)

        def copy(k, slot):
            return pltpu.make_async_remote_copy(src_ref=mine, dst_ref=slots.at[slot], send_sem=send_sem.at[k], recv_sem=recv_sem.at[slot],
                                                device_id=to(k), device_id_type=MESH)

        each(lambda k: copy(k, me).start())
        slots[pl.ds(me, 1)] = mine[:][None]
        each(lambda k: copy(k, lax.rem(me + devices - k, devices)).wait_recv())
        each(lambda k: copy(k, me).wait_send())
        out_ref[:] = jnp.minimum(1.0, 0.5 * lax.rsqrt(jnp.sum(slots[:], axis=0) / count + 1e-30))

    return _call(kernel, "clip", (), [ONCHIP] * len(grads), [ONCHIP], [_sds(block, WIDE)],
                 [pltpu.VMEM(block, WIDE), pltpu.VMEM((devices, *block), WIDE)] + [pltpu.SemaphoreType.DMA((devices,))] * 2, COST, grads, talks=talks)[0]


def adamw(factor, weights, ms, vs, grads, chips):
    steps, layers, count = 4, len(grads), len(weights)
    blocks, maps = [], []
    for w in weights:
        l, r, n = w.shape
        tall = r % (steps * 16) == 0
        blocks.append((l, r // steps, n) if tall else (l, r, n // steps))
        maps.append("a1" if tall else "a2")
    specs = [_spec(b, **{m: _first}) for b, m in zip(blocks, maps)]
    rd, ro = blocks[6][1], blocks[3][1]
    g_specs, g_args = [], []
    for qkv, rows, gu in grads:
        d = rows.shape[1]
        after = functools.partial(lambda off, i: off + i, steps * rd // ro)
        g_specs += [_spec((*qkv.shape[:2], qkv.shape[2] // steps), a2=_first), _spec((rd, d), a0=_first), _spec((ro, d), a0=after), _spec((gu.shape[0], gu.shape[1] // steps), a1=_first)]
        g_args += [qkv, rows, rows, gu]

    def kernel(factor_ref, *refs):
        ws, m_refs, v_refs, gs, outs = _split(refs, *[count] * 3, len(g_args))
        factor = factor_ref[:1, :1]
        for l in range(layers):
            (qkv, down, out, gu), gs = gs[:4], gs[4:]
            per = chips // steps
            wide = gu.shape[1] // (2 * per)
            halves = [jnp.concatenate([gu[:, pl.ds((2 * p + k) * wide, wide)] for p in range(per)], axis=1) for k in range(2)]
            for i, g in enumerate((*[qkv[k] for k in range(3)], out[:], *halves, down[:])):
                g = g.astype(WIDE) * factor
                m = 0.9 * m_refs[i][l] + 0.1 * g
                v = 0.95 * v_refs[i][l] + 0.05 * g * g
                w = ws[i][l].astype(WIDE)
                outs[i][l] = _low(w - 0.02 * (m * lax.rsqrt(v + 1e-8) + 0.1 * w))
                outs[count + i][l] = m
                outs[2 * count + i][l] = v

    shapes = [_sds(w.shape, kind) for kind in (LOW, WIDE, WIDE) for w in weights]
    return _call(kernel, "adamw", (steps,), [_spec(factor.shape)] + specs * 3 + g_specs, specs * 3, shapes, [], COST, [factor, *weights, *ms, *vs, *g_args])


def solution(mesh):
    devices = mesh.shape["dp"]
    side = math.isqrt(devices // 2)
    chips = side * side

    def step(x, dy, *arrays):
        weights, ms, vs, _ = _split(arrays, *[len(arrays) // 3] * 3)
        wq, wk, wv, wo, wg, wu, wd = weights
        layers = wq.shape[0]
        x, dy = x[0], dy[0]
        t, d = x.shape
        f, ff = wq.shape[2], wg.shape[2]
        heads = f // HEAD
        rd, ro = wd.shape[1], wo.shape[1]
        *_, c = _place()
        chip = _chip(jnp.arange(chips, dtype=jnp.int32), side)
        other = chip.reshape(side, side).T.reshape(-1)
        per = d // devices
        rel = jnp.concatenate([chip * 2 + c, other * 2 + 1 - c])
        rel = (rel[:, None] * per + jnp.arange(per, dtype=jnp.int32)).reshape(-1)
        onehot = _low(jnp.arange(d, dtype=jnp.int32)[:, None] == rel)
        relative = lambda a: _low(_dot(onehot, a, 0, 1))
        half = HEAD // 2
        angle = jnp.arange(t, dtype=WIDE)[:, None] * THETA ** (-jnp.arange(half, dtype=WIDE) / half)
        cos = jnp.concatenate([jnp.cos(angle)] * 2, 1)
        sin = jnp.concatenate([-jnp.sin(angle), jnp.sin(angle)], 1)
        gather = lambda shard: lax.all_gather(shard, "dp", axis=0, tiled=True)
        qkv_job = lambda n, *plan: Gather((wq, wk, wv), n, _plan(*plan), 6 + n, side)
        inside, joined = (wg, wu, wd), []
        joined += alone(Join(inside, 0), "joined")
        w, shard = alone(Jobs(qkv_job(0, "123456", "234567"), Join(inside, 1)), "gathered")
        w_qkv = [w.reshape(d, -1)]
        w_gu = [gather(one) for one in (*joined, shard)]
        h, kept, rows, out_w = x, [], [], []
        for n in range(layers):
            qkv = qkv_forward(h, w_qkv[n], cos, sin)
            out, out_t, lse, *more = attend(qkv, heads, None if n else Gather((wo,), n, _plan("023578"), 1, side))
            out_w += more
            rows.append(((w_gu[n], 2 * ff), (out_w[n].reshape(d, -1), 0)))
            h2, b, b_t = out_forward(h, out, rows[n][1], ro)
            kept.append((h, qkv, out_t, lse, h2, b, b_t))
            if n < layers - 1:
                jobs = Jobs(qkv_job(1, "012345", "123456"), Gather((wo,), 1, _plan("234567"), 1, side))
                h, w, more = mlp_forward(h2, b, w_gu[n], rows[n][0], rd, ff, jobs)
                w_qkv.append(w.reshape(d, -1))
                out_w.append(more)
        g_gu, g_rows, g_qkv = ([None] * layers for _ in range(3))
        scatter = lambda a: lax.psum_scatter(a, "dp", scatter_dimension=0, tiled=True)
        dh = dy
        for n in reversed(range(layers)):
            h, qkv, out_t, lse, h2, b, b_t = kept[n]
            last, job = n == 0, None
            rows_kind = lambda: Kind(pair[0].shape, 0, 1, 1, 2, side)
            if last:
                job = Exchange([pair, two], [rows_kind(), Kind(two[0].shape, 1, 2, 2, 2, side)], _plan("3579b", "468ac", "68ace", "79bdf"), 3, side)
            dh2, gu, *pair = mlp_back(h2, b, b_t, dh, w_gu[n], rows[n][0], rd, rd + ro, side, job)
            if last:
                pair, (g_rows[1], g_qkv[1]), _ = _split(pair, 2, 2)
            dot, delta, *pair = out_back(dh2, out_t, rows[n][1], ro, pair, heads, side)
            if last:
                dot, g_gu[1] = lax.optimization_barrier((dot, g_gu[1]))
            g_gu[n] = scatter(gu)
            a_rel = relative(_normed(h))
            attention = functools.partial(attend_back, qkv, dot, lse, delta, cos, sin, heads)
            if last:
                jobs = Jobs(Exchange([pair], [rows_kind()], _plan("358cf", "57bfh"), 2, side),
                            Exchange([], [Kind(two[0].shape, 1, 2, 2, 2, side)], _plan("acefg", "ghijk"), 2, side))
                g_rows[n], g_qkv[n] = attention(jobs, a_rel)
            else:
                *two, dh = qkv_back(h, a_rel, dh2, attention(), w_qkv[n])
        grads = [(g_qkv[n], g_rows[n][0], g_gu[n]) for n in range(layers)]
        factor = clip([g for one in grads for g in one], sum(w.size for w in weights) * devices, devices, 8)
        return tuple(adamw(factor, weights, ms, vs, grads, chips))

    states, cut = P(("rep", "dp"), None, None), P(None, "dp", None)
    return jax.shard_map(step, mesh=mesh, in_specs=(states, states) + (cut,) * 21, out_specs=(P("rep", "dp", None),) * 21, check_vma=False)
```
